512 devices in a mesh: tile: 64 (over z, y), level: 8 (over x, core).
Axes of the slice: x: 4, y: 4, z: 16, core: 2. Of those that a mesh axis runs over, the one named last changes fastest.
Arguments:
- anomalies: bfloat16 [512, 32, 8192], P(None, 'level', 'tile'), may hold values from -6 to 6
- footprint: bfloat16 [32768, 128], P('tile'), may hold values from -0.5 to 0.5
- weighting: float32 [32, 32768], P('level', 'tile'), may hold values from 0.02 to 0.3
- dual_rows: bfloat16 [32768, 512], P(('tile', 'level')), may hold values from -6 to 6
- taper_blocks: bfloat16 [4, 128, 512], replicated, may hold values from 0.099609375 to 1
- obs_count: int32 [64], replicated, may hold values from 1 to 512, 16384 in all
- near_tiles: int32 [64, 6], replicated, may hold values from 0 to 63, as said below
- taper_class: int32 [64, 6], P('tile'), may hold values from 0 to 3
Outputs:
- increment: float32 [512, 32, 8192], P(None, 'level', 'tile')
The draws below stay inside these ranges and needn't reach their ends.
Inputs may be any that keep to these rules, and one draw needn't show every extreme that they name: `near_tiles`: row t lists 6 different tiles, each within cyclic distance 4 of t, that is (t + d) mod 64 with |d| <= 4.
All inputs are finite; a program needn't handle non-finite values.
Results may differ from the reference program's by a relative error of at most 0.004.
Values may be sent and summed in bfloat16 or wider, within the bound.
No kernel may reach another device: no remote copies, remote signals or barrier semaphores. Data moves between devices by JAX's collectives and lax.ppermute only.
A program may use at most 64 MiB of HBM per device.

```python
import math
import jax
import jax.numpy as jnp
import numpy as np
from jax import lax

M = 512
PTS = 128
OBS_CAP = 512
NB = 6
REACH = 4
CLASSES = 4
LEV = 32
NPTS = 8192
NOBS = 32768
N_TILE = 64


def draw_near_tiles(key, part):
    keys = jax.random.split(jax.random.fold_in(key, 17), N_TILE)

    def one_row(row_key):
        return jax.random.permutation(row_key, 2 * REACH + 1)[:NB]
    offsets = jax.vmap(one_row)(keys).astype(jnp.int32) - REACH
    base_ids = jnp.arange(N_TILE, dtype=jnp.int32)[:, None]
    return ((base_ids + offsets) % N_TILE).astype(jnp.int32)


def plant(array, key, low, largest):
    index_at = [jax.random.randint(jax.random.fold_in(key, axis), (), 0, length) for axis, length in enumerate(array.shape)]
    widest = array.shape.index(max(array.shape))
    next_to = index_at[:widest] + [(index_at[widest] + 1) % array.shape[widest]] + index_at[widest + 1:]
    return array.at[tuple(index_at)].set(low).at[tuple(next_to)].set(largest)


def block_scale(stream_key, dims, cuts, smallest, top_value):
    loudness, own = 1.0, jax.random.fold_in(stream_key, 6)
    for axis_at, blocks in cuts:
        draws = jnp.exp(jax.random.uniform(jax.random.fold_in(own, axis_at), (blocks,), jnp.float32, smallest / len(cuts), top_value / len(cuts)))
        loudness = loudness * jnp.repeat(draws, dims[axis_at] // blocks).reshape([-1 if axis == axis_at else 1 for axis in range(len(dims))])
    return loudness


def profile(number_of, total, limit, slope):
    weights = [(1 << 20) // math.isqrt(standing ** slope) + 1 for standing in range(2, number_of + 1)]
    surplus, counts = total - limit - (number_of - 1), [1] * (number_of - 1)
    while surplus > 0:
        movable = [i for i in range(number_of - 1) if counts[i] < limit]
        pool, remaining = sum([weights[i] for i in movable]), surplus
        for i in movable:
            more = min(limit - counts[i], max(1, remaining * weights[i] // pool), surplus)
            counts[i] = counts[i] + more
            surplus = surplus - more
    return np.array([limit] + counts)


def uneven(own_key, amount, total, reach, skew):
    if amount == 2:
        one = jax.random.randint(own_key, (), max(1, total - reach), min(reach, total - 1) + 1)
        return jnp.stack([one, total - one])
    tallies = jnp.asarray(profile(amount, total, reach, skew), jnp.int32)
    couples = (amount - 1) // 2
    source_of, taker = tallies[1:1 + 2 * couples:2], tallies[2:2 + 2 * couples:2]
    room = jnp.minimum(source_of - 1, reach - taker)
    passed = jax.random.randint(jax.random.fold_in(own_key, 1), (couples,), 0, 1 << 20) % (room + 1)
    tallies = tallies.at[1:1 + 2 * couples:2].set(source_of - passed).at[2:2 + 2 * couples:2].set(taker + passed)
    return tallies[jax.random.permutation(jax.random.fold_in(own_key, 2), amount)]


def centred(key, extent, spread, reach, cuts=(), kind=jnp.bfloat16):
    result = spread * jax.random.normal(key, extent, jnp.float32)
    if cuts:
        result = result * block_scale(key, extent, cuts, -0.22, 0.18)
    return jnp.clip(result, -reach, reach).astype(kind)


def setup_inputs(seed: int = 0) -> dict:
    key_list = jax.random.split(jax.random.key(seed), 9)
    anomalies = centred(key_list[0], (M, LEV, NPTS), 1.0, 6.0, ((1, 8), (2, 64)))
    footprint = centred(key_list[1], (NOBS, PTS), PTS ** -0.5, 0.5, ((0, 64),))
    weighting = jnp.clip(jnp.exp(math.log(0.3) - 2.7080503 * jax.random.uniform(key_list[2], (LEV, NOBS), jnp.float32) ** block_scale(key_list[2], (LEV, NOBS), ((0, 8), (1, 64)), -0.2, 0.2)), 0.02, 0.3)
    dual_rows = centred(key_list[3], (NOBS, M), 1.0, 6.0, ((0, 512),))
    taper_blocks = jnp.clip(jax.random.uniform(key_list[4], (CLASSES, PTS, OBS_CAP), jnp.float32, 0.099609375, 1.0), 0.099609375, 1.0).astype(jnp.bfloat16)
    obs_count = uneven(key_list[5], N_TILE, N_TILE * OBS_CAP // 2, OBS_CAP, 2).astype(jnp.int32)
    near_tiles = draw_near_tiles(jax.random.fold_in(key_list[8], 71), 0)
    taper_class = plant(jax.random.randint(key_list[7], (N_TILE, NB), 0, CLASSES), jax.random.fold_in(key_list[7], 1), 0, CLASSES - 1).astype(jnp.int32)
    return dict(anomalies=anomalies, footprint=footprint, weighting=weighting, dual_rows=dual_rows, taper_blocks=taper_blocks, obs_count=obs_count, near_tiles=near_tiles, taper_class=taper_class)


def reference(anomalies, footprint, weighting, dual_rows, taper_blocks, obs_count, near_tiles, taper_class):
    def observe(tile_num):
        state = lax.dynamic_slice_in_dim(anomalies, tile_num * PTS, PTS, 2).astype(jnp.float32)
        interp = lax.dynamic_slice_in_dim(footprint, tile_num * OBS_CAP, OBS_CAP, 0).astype(jnp.float32)
        vertical = lax.dynamic_slice_in_dim(weighting, tile_num * OBS_CAP, OBS_CAP, 1)
        projected = jnp.einsum('op,mlp->lom', interp, state)
        summed = jnp.einsum('lo,lom->om', vertical, projected)
        slot_ids = jnp.arange(OBS_CAP, dtype=jnp.int32)
        present = slot_ids < obs_count[tile_num]
        return jnp.where(present[:, None], summed, jnp.float32(0.0)).astype(jnp.bfloat16)

    tile_ids = jnp.arange(N_TILE, dtype=jnp.int32)
    observed = lax.map(observe, tile_ids)
    duals = dual_rows.reshape(N_TILE, OBS_CAP, M)

    def analyse(tile_num):
        state = lax.dynamic_slice_in_dim(anomalies, tile_num * PTS, PTS, 2)
        flat_state = state.reshape(M, LEV * PTS).astype(jnp.float32)
        running = jnp.zeros((M, LEV * PTS), jnp.float32)
        for which in range(NB):
            source = near_tiles[tile_num, which]
            rows_y = lax.dynamic_index_in_dim(observed, source, 0, keepdims=False).astype(jnp.float32)
            rows_w = lax.dynamic_index_in_dim(duals, source, 0, keepdims=False).astype(jnp.float32)
            taper = lax.dynamic_index_in_dim(taper_blocks, taper_class[tile_num, which], 0, keepdims=False).astype(jnp.float32)
            covar = jnp.dot(flat_state.T, rows_y.T, preferred_element_type=jnp.float32)
            scaled = taper / jnp.float32(M - 1)
            tapered = (covar.reshape(LEV, PTS, OBS_CAP) * scaled[None]).reshape(LEV * PTS, OBS_CAP).astype(jnp.bfloat16)
            running = running + jnp.dot(rows_w.T, tapered.astype(jnp.float32).T, preferred_element_type=jnp.float32)
        return running.reshape(M, LEV, PTS)

    pieces = lax.map(analyse, tile_ids)
    return jnp.transpose(pieces, (1, 2, 0, 3)).reshape(M, LEV, NPTS)
```

```python
import functools

import jax
import jax.numpy as jnp
from jax import lax
from jax.experimental import pallas as pl
from jax.experimental.pallas import tpu as pltpu
from jax.sharding import Mesh
from jax.sharding import PartitionSpec as P

REACH = 4
F32 = jnp.float32
BF16 = jnp.bfloat16
VMEM = pl.BlockSpec(memory_space=pltpu.VMEM)
SMEM = pl.BlockSpec(memory_space=pltpu.SMEM)
NT = (((1,), (1,)), ((), ()))
RELS = 4


def cost(flops, moved):
    return pl.CostEstimate(flops=int(flops), bytes_accessed=int(moved), transcendentals=0)


def move(value, axis, steps):
    count = lax.axis_size(axis)
    return lax.ppermute(value, axis, [(i, (i + steps) % count) for i in range(count)])


def project_body(meta, foot, own, other, w_own, duals, mine, pay1, pay2, pay3, cells, a32, w_oth, acc):
    members = cells.shape[0]
    points = own.shape[1]
    levels = own.shape[0] // members
    owned = duals.shape[0]
    x, c = meta[12], meta[13]
    rows = own.shape[0]
    wide = other[rows:, :].astype(F32)
    half = wide.shape[0] // 2
    w_sum = wide[:half] + wide[half:]
    for j in range(RELS):
        w_oth[j] = w_sum[j * levels : (j + 1) * levels]
    parts = []
    columns = []
    for r in range(RELS):
        chip = lax.rem(x + r, RELS)
        start = pl.multiple_of(chip * 2 * owned + c * owned, owned)
        parts.append(foot[pl.ds(start, owned), :])
        both = jnp.concatenate([w_own[chip], w_oth[chip]], axis=0).T
        columns.append(jnp.where(c == 0, both[:owned], both[owned:]))
    picked = jnp.concatenate(parts, axis=0)
    column = jnp.concatenate(columns, axis=0)
    for h in range(2):
        a32[...] = (own if h == 0 else other)[:rows, :].astype(F32)
        for l in range(levels):
            plane = a32[pl.ds(l, members, stride=levels), :].astype(BF16)
            at = (h * levels + l) * points
            cells[:, at : at + points] = plane
            got = lax.dot_general(picked, plane, NT, preferred_element_type=F32)
            k = h * levels + l
            term = column[:, k : k + 1] * got
            if k == 0:
                acc[...] = term
            else:
                acc[...] += term
    mine[...] = acc[:owned]
    for r, pay in ((1, pay1), (2, pay2), (3, pay3)):
        pay[:owned] = acc[r * owned : (r + 1) * owned].astype(BF16)
        pay[owned:] = duals[...]


def project(meta, foot, own, other, w_own, duals):
    owned, members = duals.shape
    points = foot.shape[1]
    levels = own.shape[0] // members
    pay = jax.ShapeDtypeStruct((2 * owned, members), BF16)
    return pl.pallas_call(
        project_body,
        out_shape=(
            jax.ShapeDtypeStruct((owned, members), F32),
            pay,
            pay,
            pay,
            jax.ShapeDtypeStruct((members, 2 * levels * points), BF16),
        ),
        in_specs=[SMEM] + [VMEM] * 5,
        out_specs=(VMEM,) * 5,
        scratch_shapes=[
            pltpu.VMEM(own.shape, F32),
            pltpu.VMEM((RELS, levels, 2 * owned), F32),
            pltpu.VMEM((RELS * owned, members), F32),
        ],
        cost_estimate=cost(2 * 4 * owned * points * members * 2 * levels, 3e6),
        name="project",
    )(meta, foot, own, other, w_own, duals)


def pick_body(meta, low, mid, high, out):
    owned = out.shape[0] // 6
    for k in range(6):
        place = meta[k]
        group = place // 3
        start = pl.multiple_of(lax.rem(place, 3) * owned, owned)
        for g, source in enumerate((low, mid, high)):

            @pl.when(group == g)
            def _(source=source):
                out[k * owned : (k + 1) * owned] = source[pl.ds(start, owned), :]


def pick(meta, low, mid, high):
    members = mid.shape[1]
    return pl.pallas_call(
        pick_body,
        out_shape=jax.ShapeDtypeStruct((2 * mid.shape[0], members), BF16),
        in_specs=[SMEM] + [VMEM] * 3,
        out_specs=VMEM,
        cost_estimate=cost(1e8, 8e5),
        name="pick",
    )(meta, low, mid, high)


def prepare_body(meta, low, mid, high, taper, dual_t, scaled, sel, tall):
    x, c = meta[12], meta[13]
    members = mid.shape[1]
    owned = sel.shape[0] // 6
    classes = taper.shape[0]
    for q in range(classes):
        tall[q] = taper[q].astype(F32).T / F32(members - 1)
    for r in range(RELS):
        chip = lax.rem(x + r, RELS)
        col = pl.multiple_of(chip * 2 * owned + c * owned, owned)
        for k in range(6):
            place = meta[k]
            group = place // 3
            start = pl.multiple_of(lax.rem(place, 3) * (RELS * owned) + r * owned, owned)
            for g, source in enumerate((low, mid, high)):

                @pl.when(group == g)
                def _(source=source):
                    sel[k * owned : (k + 1) * owned] = source[pl.ds(start, owned), :]

            scaled[r, k * owned : (k + 1) * owned] = tall[meta[6 + k], pl.ds(col, owned), :]
        dual_t[r] = sel[...].T


def prepare(meta, low, mid, high, taper):
    members = mid.shape[1]
    owned = mid.shape[0] // (3 * RELS)
    classes, points, slots = taper.shape
    return pl.pallas_call(
        prepare_body,
        out_shape=(
            jax.ShapeDtypeStruct((RELS, members, 6 * owned), BF16),
            jax.ShapeDtypeStruct((RELS, 6 * owned, points), F32),
        ),
        in_specs=[SMEM] + [VMEM] * 4,
        out_specs=(VMEM, VMEM),
        scratch_shapes=[
            pltpu.VMEM((6 * owned, members), BF16),
            pltpu.VMEM((classes, slots, points), F32),
        ],
        cost_estimate=cost(3e9, 6e6),
        name="prepare",
    )(meta, low, mid, high, taper)


def analyse_body(rel, first, step, rows, cells, dual_t, scaled, *refs):
    out = refs[-1]
    before = refs[0] if len(refs) == 2 else None
    taper = scaled[rel]
    wide = jnp.concatenate([taper] * (step // taper.shape[1]), axis=1)
    for at in range(0, out.shape[1], step):
        covar = jnp.dot(rows[...], cells[:, first + at : first + at + step], preferred_element_type=F32)
        tapered = (covar * wide).astype(BF16)
        gained = jnp.dot(dual_t[rel], tapered, preferred_element_type=F32)
        if before is None:
            out[:, at : at + step] = gained
        else:
            out[:, at : at + step] = before[:, at : at + step] + gained


def analyse(rel, first, width, rows, cells, dual_t, scaled, before=None):
    members = cells.shape[0]
    inputs = [rows, cells, dual_t, scaled] + ([] if before is None else [before])
    return pl.pallas_call(
        functools.partial(analyse_body, rel, first, 256),
        out_shape=jax.ShapeDtypeStruct((members, width), F32),
        in_specs=[VMEM] * len(inputs),
        out_specs=VMEM,
        input_output_aliases={} if before is None else {4: 0},
        cost_estimate=cost(4 * rows.shape[0] * members * width, 4e6),
        name="analyse",
    )(*inputs)


def finish_body(mine, theirs, out):
    members = mine.shape[0]
    levels = out.shape[0] // members
    points = out.shape[1]
    for l in range(levels):
        at = slice(l * points, (l + 1) * points)
        out[pl.ds(l, members, stride=levels), :] = mine[:, at] + theirs[:, at]


def finish(mine, theirs, points):
    return pl.pallas_call(
        finish_body,
        out_shape=jax.ShapeDtypeStruct((mine.size // points, points), F32),
        in_specs=[VMEM] * 2,
        out_specs=VMEM,
        cost_estimate=cost(1e8, 3e6),
        name="finish",
    )(mine, theirs)


def shards(
    anomalies, footprint, weighting, dual_rows, taper_blocks, obs_count, near_tiles, taper_class
):
    members, levels, points = anomalies.shape
    owned = dual_rows.shape[0]
    tile = ("z", "y")
    tile_id = lax.axis_index(tile)
    tile_count = lax.axis_size("z") * lax.axis_size("y")
    x, c = lax.axis_index("x"), lax.axis_index("c")

    own = anomalies.reshape(members * levels, points)
    w_own = weighting.reshape(levels, RELS, 2 * owned).transpose(1, 0, 2)
    w_flat = w_own.reshape(RELS * levels, 2 * owned)
    w_high = w_flat.astype(BF16)
    w_low = (w_flat - w_high.astype(F32)).astype(BF16)
    other = move(jnp.concatenate([own, w_high, w_low], axis=0), "c", 1)

    sources = lax.dynamic_index_in_dim(near_tiles, tile_id, 0, keepdims=False)
    places = (sources - tile_id + REACH) % tile_count
    meta = jnp.concatenate([places, taper_class[0], jnp.stack([x, c])]).astype(jnp.int32)
    slot_ids = (x * 2 + c) * owned + jnp.arange(owned, dtype=jnp.int32)
    present = slot_ids < obs_count[tile_id]

    mine, pay1, pay2, pay3, cells = project(meta, footprint, own, other, w_own, dual_rows)
    got1, got3, got2 = move(pay1, "x", 1), move(pay3, "x", -1), move(pay2, "x", 2)
    observed = (
        mine + got1[:owned].astype(F32) + got3[:owned].astype(F32) + got2[:owned].astype(F32)
    )
    rows_y = jnp.where(present[:, None], observed, 0.0).astype(BF16)
    rows_w = jnp.concatenate([dual_rows, got3[owned:], got2[owned:], got1[owned:]], axis=0)

    y_low, y_high = move(rows_y, tile, 1), move(rows_y, tile, -1)
    w_low, w_high = move(rows_w, tile, 1), move(rows_w, tile, -1)
    y_mid = jnp.concatenate([y_low, rows_y, y_high], axis=0)
    w_mid = jnp.concatenate([w_low, rows_w, w_high], axis=0)
    y_far_low, y_far_high = move(y_mid, tile, 3), move(y_mid, tile, -3)
    w_far_low, w_far_high = move(w_mid, tile, 3), move(w_mid, tile, -3)

    y0 = pick(meta, y_far_low, y_mid, y_far_high)
    y3, y1, y2 = move(y0, "x", 1), move(y0, "x", -1), move(y0, "x", 2)
    dual_t, scaled = prepare(meta, w_far_low, w_mid, w_far_high, taper_blocks)

    width = levels * points
    sums = [None, None]
    for rel, rows in ((0, y0), (3, y3), (1, y1), (2, y2)):
        for h in (1, 0):
            sums[h] = analyse(rel, h * width, width, rows, cells, dual_t, scaled, sums[h])
    theirs = move(sums[1], "c", 1)
    return finish(sums[0], theirs, points).reshape(members, levels, points)


def solution(mesh):
    fine = Mesh(mesh.devices.reshape(16, 4, 4, 2), ("z", "y", "x", "c"))
    tile, level = ("z", "y"), ("x", "c")
    return jax.shard_map(
        shards,
        mesh=fine,
        in_specs=(
            P(None, level, tile),
            P(tile, None),
            P(level, tile),
            P((*tile, *level), None),
            P(),
            P(),
            P(),
            P(tile, None),
        ),
        out_specs=P(None, level, tile),
        check_vma=False,
    )
```

```python
import functools

import jax
import jax.numpy as jnp
from jax import lax
from jax.experimental import pallas as pl
from jax.experimental.pallas import tpu as pltpu
from jax.sharding import Mesh
from jax.sharding import PartitionSpec as P

REACH = 4
NEAR = 6
RELS = 4
F32 = jnp.float32
BF16 = jnp.bfloat16
VMEM = pl.BlockSpec(memory_space=pltpu.VMEM)
SMEM = pl.BlockSpec(memory_space=pltpu.SMEM)
NT = (((1,), (1,)), ((), ()))
CLASS, CHIP, CORE, LEFT = 6, 12, 13, 14


def kernel(body, out, inputs, flops, scalars=True, scratch=(), aliases=None, final=False):
    kept = [pltpu.with_memory_space_constraint(a, pltpu.VMEM) for a in inputs[scalars:]]
    shapes = [o if final else pltpu.VMEM(o.shape, o.dtype) for o in out]
    return pl.pallas_call(
        body,
        out_shape=shapes,
        in_specs=[SMEM] * scalars + [VMEM] * len(kept),
        out_specs=[VMEM] * len(out),
        scratch_shapes=list(scratch),
        input_output_aliases=aliases or {},
        cost_estimate=pl.CostEstimate(flops=int(flops), bytes_accessed=int(1e6), transcendentals=0),
        compiler_params=pltpu.CompilerParams(vmem_limit_bytes=16 << 20),
    )(*inputs[:scalars], *kept)


def array(shape, kind):
    return jax.ShapeDtypeStruct(shape, kind)


def move(value, axis, steps):
    count = lax.axis_size(axis)
    return lax.ppermute(value, axis, [(i, (i + steps) % count) for i in range(count)])


def pack_body(raw, weights, out, wide):
    members = out.shape[0] - 16
    levels, slots = weights.shape
    points = raw.shape[1]
    wide[...] = raw[...].astype(F32)
    for l in range(levels):
        plane = wide[pl.ds(l, members, stride=levels), :].astype(BF16)
        out[:members, l * points : (l + 1) * points] = plane
    high = weights[...].astype(BF16).astype(F32)
    low = weights[...] - high
    pad = jnp.zeros((16 - 2 * levels, slots), F32)
    out[members:, :] = jnp.concatenate([high, low, pad], axis=0).astype(BF16)


def columns(meta, weights, owned):
    parts = []
    for r in range(RELS):
        chip = lax.rem(meta[CHIP] + r, RELS)
        block = weights(pl.ds(pl.multiple_of(chip * 2 * owned, 2 * owned), 2 * owned))
        flipped = jnp.concatenate([block, block], axis=0).T
        parts.append(jnp.where(meta[CORE] == 0, flipped[:owned], flipped[owned:]))
    return jnp.concatenate(parts, axis=0)


def rows_of(meta, foot, owned):
    parts = []
    for r in range(RELS):
        chip = lax.rem(meta[CHIP] + r, RELS)
        start = pl.multiple_of(chip * 2 * owned + meta[CORE] * owned, owned)
        parts.append(foot[pl.ds(start, owned), :])
    return jnp.concatenate(parts, axis=0)


def project(picked, column, cells, acc, fresh):
    members = acc.shape[1]
    points = picked.shape[1]
    for l in range(cells.shape[1] // points):
        plane = cells[:members, l * points : (l + 1) * points]
        got = lax.dot_general(picked, plane, NT, preferred_element_type=F32)
        term = column[:, l : l + 1] * got
        if l == 0 and fresh:
            acc[...] = term
        else:
            acc[...] += term


def own_body(meta, foot, cells, weights, out):
    owned = out.shape[0] // RELS
    column = columns(meta, lambda at: weights[:, at], owned)
    project(rows_of(meta, foot, owned), column, cells, out, True)


def other_body(meta, foot, cells, before, duals, mine, pay1, pay2, pay3, acc):
    owned, members = duals.shape

    def weights(at):
        terms = cells[members:, at].astype(F32)
        return terms[:4] + terms[4:8]

    acc[...] = before[...]
    project(rows_of(meta, foot, owned), columns(meta, weights, owned), cells, acc, False)
    mine[...] = acc[:owned]
    for r, pay in ((1, pay1), (2, pay2), (3, pay3)):
        part = acc[r * owned : (r + 1) * owned]
        high = part.astype(BF16)
        pay[:owned] = high
        pay[owned : 2 * owned] = (part - high.astype(F32)).astype(BF16)
        pay[2 * owned :] = duals[...]


def fold_body(meta, mine, *refs):
    out = refs[-1]
    owned = out.shape[0]
    total = mine[...]
    for got in refs[:-1]:
        total = total + (got[:owned].astype(F32) + got[owned : 2 * owned].astype(F32))
    slot = lax.broadcasted_iota(jnp.int32, total.shape, 0)
    out[...] = jnp.where(slot < meta[LEFT], total, 0.0).astype(BF16)


def flip_body(duals, after, across, before, out):
    owned = duals.shape[0]
    rows = [duals[...]] + [got[2 * owned :] for got in (after, across, before)]
    out[...] = jnp.concatenate(rows, axis=0).T


def choose(meta, k, sources, size, store):
    group = meta[k] // 3
    start = pl.multiple_of(lax.rem(meta[k], 3) * size, size)
    for g, source in enumerate(sources):

        @pl.when(group == g)
        def _(source=source):
            store(source[pl.ds(start, size), :])


def pick_body(meta, low, mid, high, out):
    size = out.shape[0] // NEAR
    for k in range(NEAR):

        def store(value, k=k):
            out[k * size : (k + 1) * size] = value

        choose(meta, k, (low, mid, high), size, store)


def pick_dual_body(meta, low, mid, high, out):
    size = out.shape[0]
    wide = out.shape[1] // NEAR
    for k in range(NEAR):

        def store(value, k=k):
            out[:, k * wide : (k + 1) * wide] = value

        choose(meta, k, (low, mid, high), size, store)


def taper_body(meta, taper, out, tall):
    classes = taper.shape[0]
    owned = out.shape[1] // NEAR
    for q in range(classes):
        tall[q] = taper[q].astype(F32).T / F32(511)
    for r in range(RELS):
        chip = lax.rem(meta[CHIP] + r, RELS)
        start = pl.multiple_of(chip * 2 * owned + meta[CORE] * owned, owned)
        for k in range(NEAR):
            out[r, k * owned : (k + 1) * owned] = tall[meta[CLASS + k], pl.ds(start, owned), :]


def covary_body(rel, rows, own, other, scaled, *refs):
    out = refs[-1]
    members = rows.shape[1]
    size = rows.shape[0] // NEAR
    half = own.shape[1]
    step = 256
    taper = scaled[rel]
    wide = jnp.concatenate([taper] * (step // taper.shape[1]), axis=1)
    for h, cells in enumerate((own, other)):
        for at in range(0, half, step):
            covar = jnp.dot(rows[...], cells[:members, at : at + step], preferred_element_type=F32)
            tapered = (covar * wide).astype(BF16)
            for k in range(NEAR):
                first = (k * RELS + rel) * size
                out[first : first + size, h * half + at : h * half + at + step] = tapered[
                    k * size : (k + 1) * size
                ]


def gain_body(h, duals, tapered, out):
    half = out.shape[1]
    step = 256
    for at in range(0, half, step):
        out[:, at : at + step] = jnp.dot(
            duals[...], tapered[:, h * half + at : h * half + at + step], preferred_element_type=F32
        )


def finish_body(mine, theirs, out):
    members = mine.shape[0]
    levels = out.shape[0] // members
    points = out.shape[1]
    for l in range(levels):
        at = slice(l * points, (l + 1) * points)
        out[pl.ds(l, members, stride=levels), :] = mine[:, at] + theirs[:, at]


def shards(
    anomalies, footprint, weighting, dual_rows, taper_blocks, obs_count, near_tiles, taper_class
):
    members, levels, points = anomalies.shape
    owned = dual_rows.shape[0]
    tile = ("z", "y")
    tile_id = lax.axis_index(tile)
    tile_count = lax.axis_size("z") * lax.axis_size("y")
    x, c = lax.axis_index("x"), lax.axis_index("c")

    raw = anomalies.reshape(members * levels, points)
    (own,) = kernel(
        pack_body,
        [array((members + 16, levels * points), BF16)],
        [raw, weighting],
        1e8,
        scalars=False,
        scratch=[pltpu.VMEM(raw.shape, F32)],
    )
    other = move(own, "c", 1)

    sources = lax.dynamic_index_in_dim(near_tiles, tile_id, 0, keepdims=False)
    places = (sources - tile_id + REACH) % tile_count
    left = obs_count[tile_id] - (x * 2 + c) * owned
    meta = jnp.concatenate([places, taper_class[0], jnp.stack([x, c, left, left])]).astype(jnp.int32)

    rows = RELS * owned
    work = 2 * rows * points * members * levels
    (begun,) = kernel(
        own_body, [array((rows, members), F32)], [meta, footprint, own, weighting], work
    )
    pay = array((3 * owned, members), BF16)
    mine, pay1, pay2, pay3 = kernel(
        other_body,
        [array((owned, members), F32), pay, pay, pay],
        [meta, footprint, other, begun, dual_rows],
        work,
        scratch=[pltpu.VMEM((rows, members), F32)],
    )
    got1, got3, got2 = move(pay1, "x", 1), move(pay3, "x", -1), move(pay2, "x", 2)
    (rows_y,) = kernel(
        fold_body, [array((owned, members), BF16)], [meta, mine, got1, got3, got2], 1e8
    )
    y_low, y_high = move(rows_y, tile, 1), move(rows_y, tile, -1)
    (dual_t,) = kernel(
        flip_body, [array((members, rows), BF16)], [dual_rows, got3, got2, got1], 1e8, scalars=False
    )
    y_mid = jnp.concatenate([y_low, rows_y, y_high], axis=0)
    y_far_low, y_far_high = move(y_mid, tile, 3), move(y_mid, tile, -3)
    w_low, w_high = move(dual_t, tile, 1), move(dual_t, tile, -1)
    (y0,) = kernel(
        pick_body, [array((NEAR * owned, members), BF16)], [meta, y_far_low, y_mid, y_far_high], 1e8
    )
    y3, y1, y2 = move(y0, "x", 1), move(y0, "x", -1), move(y0, "x", 2)
    w_mid = jnp.concatenate([w_low, dual_t, w_high], axis=0)
    w_far_low, w_far_high = move(w_mid, tile, 3), move(w_mid, tile, -3)

    meta_late, _ = lax.optimization_barrier((meta, y0))
    (scaled,) = kernel(
        taper_body,
        [array((RELS, NEAR * owned, points), F32)],
        [meta_late, taper_blocks],
        1e9,
        scratch=[pltpu.VMEM((taper_blocks.shape[0], taper_blocks.shape[2], points), F32)],
    )
    width = levels * points
    tapered = None
    for rel, got in ((0, y0), (3, y3), (1, y1), (2, y2)):
        inputs = [got, own, other, scaled] + ([] if tapered is None else [tapered])
        (tapered,) = kernel(
            functools.partial(covary_body, rel),
            [array((NEAR * rows, 2 * width), BF16)],
            inputs,
            4 * NEAR * owned * members * width,
            scalars=False,
            aliases={} if tapered is None else {4: 0},
        )
    (duals,) = kernel(
        pick_dual_body,
        [array((members, NEAR * rows), BF16)],
        [meta, w_far_low, w_mid, w_far_high],
        1e8,
    )
    sums = [
        kernel(
            functools.partial(gain_body, h),
            [array((members, width), F32)],
            [duals, tapered],
            2 * NEAR * rows * members * width,
            scalars=False,
        )[0]
        for h in (0, 1)
    ]
    theirs = move(sums[1], "c", 1)
    (out,) = kernel(
        finish_body,
        [array((members * levels, points), F32)],
        [sums[0], theirs],
        1e8,
        scalars=False,
        final=True,
    )
    return out.reshape(members, levels, points)


def solution(mesh):
    fine = Mesh(mesh.devices.reshape(16, 4, 4, 2), ("z", "y", "x", "c"))
    tile, level = ("z", "y"), ("x", "c")
    return jax.shard_map(
        shards,
        mesh=fine,
        in_specs=(
            P(None, level, tile),
            P(tile, None),
            P(level, tile),
            P((*tile, *level), None),
            P(),
            P(),
            P(),
            P(tile, None),
        ),
        out_specs=P(None, level, tile),
        check_vma=False,
    )
```

```python
import functools

import jax
import jax.numpy as jnp
from jax import lax
from jax.experimental import pallas as pl
from jax.experimental.pallas import tpu as pltpu
from jax.sharding import Mesh
from jax.sharding import PartitionSpec as P

REACH = 4
NEAR = 6
RELS = 4
F32 = jnp.float32
BF16 = jnp.bfloat16
NT = (((1,), (1,)), ((), ()))
CLASS, CHIP, CORE, COUNT = 6, 12, 13, 14


def kernel(body, out, inputs, flops, scalars=0, scratch=(), aliases=None, given=None, spaces=None):
    spaces = spaces or [pltpu.VMEM] * len(out)
    given = given or [pltpu.SMEM] * scalars + [pltpu.VMEM] * (len(inputs) - scalars)
    inputs = [pltpu.with_memory_space_constraint(a, m) for a, m in zip(inputs, given)]
    return pl.pallas_call(
        body,
        out_shape=[o if m is None else m(o.shape, o.dtype) for o, m in zip(out, spaces)],
        in_specs=[pl.BlockSpec(memory_space=m) for m in given],
        out_specs=[pl.BlockSpec(memory_space=m or pl.ANY) for m in spaces],
        scratch_shapes=list(scratch),
        input_output_aliases=aliases or {},
        cost_estimate=pl.CostEstimate(flops=int(flops), bytes_accessed=int(1e6), transcendentals=0),
        compiler_params=pltpu.CompilerParams(vmem_limit_bytes=16 << 20),
    )(*inputs)


def array(shape, kind):
    return jax.ShapeDtypeStruct(shape, kind)


def move(value, axis, steps):
    count = lax.axis_size(axis)
    return lax.ppermute(value, axis, [(i, (i + steps) % count) for i in range(count)])


def pack_body(*refs):
    given, (meta, out, weights, foot), held = refs[:6], refs[6:10], refs[10:]
    near, count, classes, raw, wide, done = held
    copies = []
    for q, kept in enumerate((near, count, classes, raw, weights, foot)):
        copies.append(pltpu.make_async_copy(given[q], kept, done.at[q]))
    for q in (3, 4, 0, 1, 2, 5):
        copies[q].start()
    copies[3].wait()
    members = out.shape[0] - 16
    levels, slots = weights.shape
    points = raw.shape[1]
    wide[...] = raw[...].astype(F32)
    for l in range(levels):
        plane = wide[pl.ds(l, members, stride=levels), :].astype(BF16)
        out[:members, l * points : (l + 1) * points] = plane
    for q in (4, 0, 1, 2, 5):
        copies[q].wait()
    high = weights[...].astype(BF16).astype(F32)
    low = weights[...] - high
    pad = jnp.zeros((16 - 2 * levels, slots), F32)
    out[members:, :] = jnp.concatenate([high, low, pad], axis=0).astype(BF16)
    tile = lax.axis_index("z") * lax.axis_size("y") + lax.axis_index("y")
    tiles = lax.axis_size("z") * lax.axis_size("y")
    for k in range(NEAR):
        meta[k] = lax.rem(near[k, tile] - tile + REACH + tiles, tiles)
        meta[CLASS + k] = classes[0, k]
    meta[CHIP] = lax.axis_index("x")
    meta[CORE] = lax.axis_index("c")
    meta[COUNT] = count[tile]


def columns(meta, weights, owned):
    parts = []
    for r in range(RELS):
        chip = lax.rem(meta[CHIP] + r, RELS)
        block = weights(pl.ds(pl.multiple_of(chip * 2 * owned, 2 * owned), 2 * owned))
        flipped = jnp.concatenate([block, block], axis=0).T
        parts.append(jnp.where(meta[CORE] == 0, flipped[:owned], flipped[owned:]))
    return jnp.concatenate(parts, axis=0)


def rows_of(meta, foot, owned):
    parts = []
    for r in range(RELS):
        chip = lax.rem(meta[CHIP] + r, RELS)
        start = pl.multiple_of(chip * 2 * owned + meta[CORE] * owned, owned)
        parts.append(foot[pl.ds(start, owned), :])
    return jnp.concatenate(parts, axis=0)


def project(picked, column, cells, acc, fresh):
    members = acc.shape[1]
    points = picked.shape[1]
    for l in range(cells.shape[1] // points):
        plane = cells[:members, l * points : (l + 1) * points]
        got = lax.dot_general(picked, plane, NT, preferred_element_type=F32)
        term = column[:, l : l + 1] * got
        if l == 0 and fresh:
            acc[...] = term
        else:
            acc[...] += term


def own_body(meta, foot, cells, weights, out):
    owned = out.shape[0] // RELS
    column = columns(meta, lambda at: weights[:, at], owned)
    project(rows_of(meta, foot, owned), column, cells, out, True)


def other_body(meta, foot, cells, before, mine, pay1, pay2, pay3, acc):
    owned, members = mine.shape

    def weights(at):
        terms = cells[members:, at].astype(F32)
        return terms[:4] + terms[4:8]

    acc[...] = before[...]
    project(rows_of(meta, foot, owned), columns(meta, weights, owned), cells, acc, False)
    slot = lax.broadcasted_iota(jnp.int32, mine.shape, 0) + meta[CORE] * owned
    for r, pay in enumerate((mine, pay1, pay2, pay3)):
        chip = lax.rem(meta[CHIP] + r, RELS)
        present = slot + chip * 2 * owned < meta[COUNT]
        part = jnp.where(present, acc[r * owned : (r + 1) * owned], 0.0)
        if r == 0:
            mine[...] = part
        else:
            high = part.astype(BF16)
            pay[:owned] = high
            pay[owned:] = (part - high.astype(F32)).astype(BF16)


def fold_body(mine, *refs):
    out = refs[-1]
    owned = out.shape[0]
    total = mine[...]
    for got in refs[:-1]:
        total = total + (got[:owned].astype(F32) + got[owned:].astype(F32))
    out[...] = total.astype(BF16)


def flip_body(*refs):
    out = refs[-1]
    wide = refs[0].shape[0]
    for r, rows in enumerate(refs[:-1]):
        out[:, r * wide : (r + 1) * wide] = rows[...].T


def choose(meta, k, sources, size, store):
    group = meta[k] // 3
    start = pl.multiple_of(lax.rem(meta[k], 3) * size, size)
    for g, source in enumerate(sources):

        @pl.when(group == g)
        def _(source=source):
            store(source[pl.ds(start, size), :])


def pick_body(meta, low, mid, high, out):
    size = out.shape[0] // NEAR
    for k in range(NEAR):

        def store(value, k=k):
            out[k * size : (k + 1) * size] = value

        choose(meta, k, (low, mid, high), size, store)


def taper_body(meta, taper, out, tall):
    classes = taper.shape[0]
    owned = out.shape[1] // NEAR
    for q in range(classes):
        tall[q] = taper[q].astype(F32).T / F32(511)
    for r in range(RELS):
        chip = lax.rem(meta[CHIP] + r, RELS)
        start = pl.multiple_of(chip * 2 * owned + meta[CORE] * owned, owned)
        for k in range(NEAR):
            out[r, k * owned : (k + 1) * owned] = tall[meta[CLASS + k], pl.ds(start, owned), :]


def covary_body(rel, rows, own, other, scaled, *refs):
    out = refs[-1]
    members = rows.shape[1]
    size = rows.shape[0]
    half = own.shape[1]
    step = 256
    taper = scaled[rel]
    wide = jnp.concatenate([taper] * (step // taper.shape[1]), axis=1)
    for h, cells in enumerate((own, other)):
        for at in range(0, half, step):
            covar = jnp.dot(rows[...], cells[:members, at : at + step], preferred_element_type=F32)
            tapered = (covar * wide).astype(BF16)
            out[rel * size : (rel + 1) * size, h * half + at : h * half + at + step] = tapered


def gain_body(h, duals, tapered, out):
    half = out.shape[1]
    step = 256
    for at in range(0, half, step):
        out[:, at : at + step] = jnp.dot(
            duals[...], tapered[:, h * half + at : h * half + at + step], preferred_element_type=F32
        )


def finish_body(mine, theirs, out, held, done):
    members = mine.shape[0]
    levels = out.shape[0] // members
    points = out.shape[1]
    parts = done.shape[0]
    size = members // parts
    copies = []
    for q in range(parts):
        for l in range(levels):
            at = (slice(q * size, (q + 1) * size), slice(l * points, (l + 1) * points))
            held[pl.ds(q * size * levels + l, size, stride=levels), :] = mine[at] + theirs[at]
        span = pl.ds(q * size * levels, size * levels)
        copies.append(pltpu.make_async_copy(held.at[span], out.at[span], done.at[q]))
        copies[-1].start()
    for copy in copies:
        copy.wait()


def shards(
    anomalies, footprint, weighting, dual_rows, taper_blocks, obs_count, near_tiles, taper_class
):
    members, levels, points = anomalies.shape
    owned = dual_rows.shape[0]
    tile = ("z", "y")
    w_low, w_high = move(dual_rows, tile, 1), move(dual_rows, tile, -1)
    raw = anomalies.reshape(members * levels, points)
    meta, own, weights, foot = kernel(
        pack_body,
        [
            array((16,), jnp.int32),
            array((members + 16, levels * points), BF16),
            array(weighting.shape, F32),
            array(footprint.shape, BF16),
        ],
        [near_tiles.T, obs_count, taper_class, raw, weighting, footprint],
        1e8,
        scratch=[
            pltpu.SMEM(near_tiles.T.shape, jnp.int32),
            pltpu.SMEM(obs_count.shape, jnp.int32),
            pltpu.SMEM(taper_class.shape, jnp.int32),
            pltpu.VMEM(raw.shape, BF16),
            pltpu.VMEM(raw.shape, F32),
            pltpu.SemaphoreType.DMA((6,)),
        ],
        given=[pltpu.HBM] * 6,
        spaces=[pltpu.SMEM, pltpu.VMEM, pltpu.VMEM, pltpu.VMEM],
    )
    other = move(own, "c", 1)

    rows = RELS * owned
    work = 2 * rows * points * members * levels
    (begun,) = kernel(
        own_body, [array((rows, members), F32)], [meta, foot, own, weights], work, scalars=1
    )
    pay = array((2 * owned, members), BF16)
    mine, pay1, pay2, pay3 = kernel(
        other_body,
        [array((owned, members), F32), pay, pay, pay],
        [meta, foot, other, begun],
        work,
        scalars=1,
        scratch=[pltpu.VMEM((rows, members), F32)],
    )
    got1, got3, got2 = move(pay1, "x", 1), move(pay3, "x", -1), move(pay2, "x", 2)
    w_mid = jnp.concatenate([w_low, dual_rows, w_high], axis=0)
    w_far_low, w_far_high = move(w_mid, tile, 3), move(w_mid, tile, -3)
    (rows_y,) = kernel(fold_body, [array((owned, members), BF16)], [mine, got1, got3, got2], 1e8)
    y_low, y_high = move(rows_y, tile, 1), move(rows_y, tile, -1)
    chosen = [array((NEAR * owned, members), BF16)]
    (w0,) = kernel(pick_body, chosen, [meta, w_far_low, w_mid, w_far_high], 1e8, scalars=1)
    w3, w1, w2 = move(w0, "x", 1), move(w0, "x", -1), move(w0, "x", 2)
    y_mid = jnp.concatenate([y_low, rows_y, y_high], axis=0)
    y_far_low, y_far_high = move(y_mid, tile, 3), move(y_mid, tile, -3)
    (y0,) = kernel(pick_body, chosen, [meta, y_far_low, y_mid, y_far_high], 1e8, scalars=1)
    y3, y1, y2 = move(y0, "x", 1), move(y0, "x", -1), move(y0, "x", 2)

    taper_late, _ = lax.optimization_barrier((taper_blocks, y0))
    (scaled,) = kernel(
        taper_body,
        [array((RELS, NEAR * owned, points), F32)],
        [meta, taper_late],
        1e9,
        scalars=1,
        scratch=[pltpu.VMEM((taper_blocks.shape[0], taper_blocks.shape[2], points), F32)],
    )
    width = levels * points
    tapered = None
    for rel, got in ((0, y0), (3, y3), (1, y1), (2, y2)):
        inputs = [got, own, other, scaled] + ([] if tapered is None else [tapered])
        (tapered,) = kernel(
            functools.partial(covary_body, rel),
            [array((NEAR * rows, 2 * width), BF16)],
            inputs,
            4 * NEAR * owned * members * width,
            aliases={} if tapered is None else {4: 0},
        )
    (duals,) = kernel(flip_body, [array((members, NEAR * rows), BF16)], [w0, w1, w2, w3], 1e9)
    sums = [
        kernel(
            functools.partial(gain_body, h),
            [array((members, width), F32)],
            [duals, tapered],
            2 * NEAR * rows * members * width,
        )[0]
        for h in (0, 1)
    ]
    theirs = move(sums[1], "c", 1)
    (out,) = kernel(
        finish_body,
        [array((members * levels, points), F32)],
        [sums[0], theirs],
        1e8,
        scratch=[pltpu.VMEM((members * levels, points), F32), pltpu.SemaphoreType.DMA((4,))],
        spaces=[None],
    )
    return out.reshape(members, levels, points)


def solution(mesh):
    fine = Mesh(mesh.devices.reshape(16, 4, 4, 2), ("z", "y", "x", "c"))
    tile, level = ("z", "y"), ("x", "c")
    return jax.shard_map(
        shards,
        mesh=fine,
        in_specs=(
            P(None, level, tile),
            P(tile, None),
            P(level, tile),
            P((*tile, *level), None),
            P(),
            P(),
            P(),
            P(tile, None),
        ),
        out_specs=P(None, level, tile),
        check_vma=False,
    )
```

```python
import functools

import jax
import jax.numpy as jnp
from jax import lax
from jax.experimental import pallas as pl
from jax.experimental.pallas import tpu as pltpu
from jax.sharding import Mesh
from jax.sharding import PartitionSpec as P

REACH = 4
NEAR = 6
RELS = 4
F32 = jnp.float32
BF16 = jnp.bfloat16
NT = (((1,), (1,)), ((), ()))
CLASS, CHIP, CORE, COUNT = 6, 12, 13, 14


def kernel(body, out, inputs, flops, scalars=0, scratch=(), aliases=None, given=None, spaces=None):
    spaces = spaces or [pltpu.VMEM] * len(out)
    given = given or [pltpu.SMEM] * scalars + [pltpu.VMEM] * (len(inputs) - scalars)
    inputs = [pltpu.with_memory_space_constraint(a, m) for a, m in zip(inputs, given)]
    return pl.pallas_call(
        body,
        out_shape=[o if m is None else m(o.shape, o.dtype) for o, m in zip(out, spaces)],
        in_specs=[pl.BlockSpec(memory_space=m) for m in given],
        out_specs=[pl.BlockSpec(memory_space=m or pl.ANY) for m in spaces],
        scratch_shapes=list(scratch),
        input_output_aliases=aliases or {},
        cost_estimate=pl.CostEstimate(flops=int(flops), bytes_accessed=int(1e6), transcendentals=0),
        compiler_params=pltpu.CompilerParams(vmem_limit_bytes=16 << 20),
    )(*inputs)


def array(shape, kind):
    return jax.ShapeDtypeStruct(shape, kind)


def move(value, axis, steps):
    count = lax.axis_size(axis)
    return lax.ppermute(value, axis, [(i, (i + steps) % count) for i in range(count)])


def pack_body(*refs):
    given, (meta, out, weights, foot), held = refs[:6], refs[6:10], refs[10:]
    near, count, classes, raw, wide, done = held
    copies = []
    for q, kept in enumerate((near, count, classes, raw, weights, foot)):
        copies.append(pltpu.make_async_copy(given[q], kept, done.at[q]))
    for q in (3, 4, 0, 1, 2, 5):
        copies[q].start()
    copies[3].wait()
    members = out.shape[0] - 16
    levels, slots = weights.shape
    points = raw.shape[1]
    wide[...] = raw[...].astype(F32)
    for l in range(levels):
        plane = wide[pl.ds(l, members, stride=levels), :].astype(BF16)
        out[:members, l * points : (l + 1) * points] = plane
    for q in (4, 0, 1, 2, 5):
        copies[q].wait()
    high = weights[...].astype(BF16).astype(F32)
    low = weights[...] - high
    pad = jnp.zeros((16 - 2 * levels, slots), F32)
    out[members:, :] = jnp.concatenate([high, low, pad], axis=0).astype(BF16)
    tile = lax.axis_index("z") * lax.axis_size("y") + lax.axis_index("y")
    tiles = lax.axis_size("z") * lax.axis_size("y")
    for k in range(NEAR):
        meta[k] = lax.rem(near[k, tile] - tile + REACH + tiles, tiles)
        meta[CLASS + k] = classes[0, k]
    meta[CHIP] = lax.axis_index("x")
    meta[CORE] = lax.axis_index("c")
    meta[COUNT] = count[tile]


def columns(meta, weights, owned):
    parts = []
    for chip in range(RELS):
        block = weights(slice(chip * 2 * owned, (chip + 1) * 2 * owned))
        flipped = jnp.concatenate([block, block], axis=0).T
        parts.append(jnp.where(meta[CORE] == 0, flipped[:owned], flipped[owned:]))
    return jnp.concatenate(parts, axis=0)


def rows_of(meta, foot, owned):
    parts = []
    for chip in range(RELS):
        start = pl.multiple_of(chip * 2 * owned + meta[CORE] * owned, owned)
        parts.append(foot[pl.ds(start, owned), :])
    return jnp.concatenate(parts, axis=0)


def project(picked, column, cells, acc, fresh):
    members = acc.shape[1]
    points = picked.shape[1]
    for l in range(cells.shape[1] // points):
        plane = cells[:members, l * points : (l + 1) * points]
        got = lax.dot_general(picked, plane, NT, preferred_element_type=F32)
        term = column[:, l : l + 1] * got
        if l == 0 and fresh:
            acc[...] = term
        else:
            acc[...] += term


def own_body(meta, foot, cells, weights, out):
    owned = out.shape[0] // RELS
    column = columns(meta, lambda at: weights[:, at], owned)
    project(rows_of(meta, foot, owned), column, cells, out, True)


def other_body(meta, foot, cells, before, pay, acc):
    members = acc.shape[1]
    owned = acc.shape[0] // RELS

    def weights(at):
        terms = cells[members:, at].astype(F32)
        return terms[:4] + terms[4:8]

    acc[...] = before[...]
    project(rows_of(meta, foot, owned), columns(meta, weights, owned), cells, acc, False)
    slot = lax.broadcasted_iota(jnp.int32, (owned, members), 0) + meta[CORE] * owned
    for chip in range(RELS):
        present = slot + chip * 2 * owned < meta[COUNT]
        part = jnp.where(present, acc[chip * owned : (chip + 1) * owned], 0.0)
        high = part.astype(BF16)
        pay[chip, :owned] = high
        pay[chip, owned:] = (part - high.astype(F32)).astype(BF16)


def fold_body(got, duals, out):
    owned = duals.shape[0]
    total = got[0, :owned].astype(F32) + got[0, owned:].astype(F32)
    for chip in range(1, RELS):
        total = total + (got[chip, :owned].astype(F32) + got[chip, owned:].astype(F32))
    out[:owned] = total.astype(BF16)
    out[owned:] = duals[...]


def pick_body(meta, low, mid, high, out):
    size = out.shape[0] // (2 * NEAR)
    for k in range(NEAR):
        group = meta[k] // 3
        start = pl.multiple_of(lax.rem(meta[k], 3) * (2 * size), 2 * size)
        for g, source in enumerate((low, mid, high)):

            @pl.when(group == g)
            def _(k=k, start=start, source=source):
                out[k * size : (k + 1) * size] = source[pl.ds(start, size), :]
                at = (NEAR + k) * size
                out[at : at + size] = source[pl.ds(pl.multiple_of(start + size, size), size), :]


def taper_body(meta, taper, out, tall):
    classes = taper.shape[0]
    owned = out.shape[1] // NEAR
    for q in range(classes):
        tall[q] = taper[q].astype(F32).T / F32(511)
    for r in range(RELS):
        chip = lax.rem(meta[CHIP] + r, RELS)
        start = pl.multiple_of(chip * 2 * owned + meta[CORE] * owned, owned)
        for k in range(NEAR):
            out[r, k * owned : (k + 1) * owned] = tall[meta[CLASS + k], pl.ds(start, owned), :]


def analyse_body(rel, halves, rows, scaled, *refs):
    count = len(halves)
    cells, before = refs[:count], refs[count:-count - 1]
    outs, flipped = refs[-count - 1 : -1], refs[-1]
    members = rows.shape[1]
    size = rows.shape[0] // 2
    step = 256
    taper = scaled[rel]
    wide = jnp.concatenate([taper] * (step // taper.shape[1]), axis=1)
    flipped[...] = rows[size:, :].T
    for h in range(count):
        for at in range(0, outs[h].shape[1], step):
            span = slice(at, at + step)
            covar = jnp.dot(rows[:size], cells[h][:members, span], preferred_element_type=F32)
            tapered = (covar * wide).astype(BF16)
            gained = jnp.dot(flipped[...], tapered, preferred_element_type=F32)
            outs[h][:, span] = before[h][:, span] + gained if before else gained


def finish_body(mine, theirs, out, held, done):
    members = mine.shape[0]
    levels = out.shape[0] // members
    points = out.shape[1]
    parts = done.shape[0]
    size = members // parts
    copies = []
    for q in range(parts):
        for l in range(levels):
            at = (slice(q * size, (q + 1) * size), slice(l * points, (l + 1) * points))
            held[pl.ds(q * size * levels + l, size, stride=levels), :] = mine[at] + theirs[at]
        span = pl.ds(q * size * levels, size * levels)
        copies.append(pltpu.make_async_copy(held.at[span], out.at[span], done.at[q]))
        copies[-1].start()
    for copy in copies:
        copy.wait()


def shards(
    anomalies, footprint, weighting, dual_rows, taper_blocks, obs_count, near_tiles, taper_class
):
    members, levels, points = anomalies.shape
    owned = dual_rows.shape[0]
    tile = ("z", "y")
    raw = anomalies.reshape(members * levels, points)
    meta, own, weights, foot = kernel(
        pack_body,
        [
            array((16,), jnp.int32),
            array((members + 16, levels * points), BF16),
            array(weighting.shape, F32),
            array(footprint.shape, BF16),
        ],
        [near_tiles.T, obs_count, taper_class, raw, weighting, footprint],
        1e8,
        scratch=[
            pltpu.SMEM(near_tiles.T.shape, jnp.int32),
            pltpu.SMEM(obs_count.shape, jnp.int32),
            pltpu.SMEM(taper_class.shape, jnp.int32),
            pltpu.VMEM(raw.shape, BF16),
            pltpu.VMEM(raw.shape, F32),
            pltpu.SemaphoreType.DMA((6,)),
        ],
        given=[pltpu.HBM] * 6,
        spaces=[pltpu.SMEM, pltpu.VMEM, pltpu.VMEM, pltpu.VMEM],
    )
    other = move(own, "c", 1)

    rows = RELS * owned
    work = 2 * rows * points * members * levels
    (begun,) = kernel(
        own_body, [array((rows, members), F32)], [meta, foot, own, weights], work, scalars=1
    )
    (pay,) = kernel(
        other_body,
        [array((RELS, 2 * owned, members), BF16)],
        [meta, foot, other, begun],
        work,
        scalars=1,
        scratch=[pltpu.VMEM((rows, members), F32)],
    )
    got = lax.all_to_all(pay, "x", 0, 0, tiled=True)
    (here,) = kernel(fold_body, [array((2 * owned, members), BF16)], [got, dual_rows], 1e8)
    low, high = move(here, tile, 1), move(here, tile, -1)
    mid = jnp.concatenate([low, here, high], axis=0)
    far_low, far_high = move(mid, tile, 3), move(mid, tile, -3)
    (y0,) = kernel(
        pick_body,
        [array((2 * NEAR * owned, members), BF16)],
        [meta, far_low, mid, far_high],
        1e8,
        scalars=1,
    )
    y3, y1, y2 = move(y0, "x", 1), move(y0, "x", -1), move(y0, "x", 2)

    taper_late, _ = lax.optimization_barrier((taper_blocks, y0))
    (scaled,) = kernel(
        taper_body,
        [array((RELS, NEAR * owned, points), F32)],
        [meta, taper_late],
        1e9,
        scalars=1,
        scratch=[pltpu.VMEM((taper_blocks.shape[0], taper_blocks.shape[2], points), F32)],
    )
    width = levels * points
    sums = [None, None]
    planes = [own, other]
    for rel, got, halves in (
        (0, y0, (0, 1)),
        (3, y3, (0, 1)),
        (1, y1, (0, 1)),
        (2, y2, (1,)),
        (2, y2, (0,)),
    ):
        cells = [planes[h] for h in halves]
        before = [sums[h] for h in halves if sums[h] is not None]
        gained = kernel(
            functools.partial(analyse_body, rel, halves),
            [array((members, width), F32)] * len(halves),
            [got, scaled, *cells, *before],
            4 * NEAR * owned * members * width * len(halves),
            scratch=[pltpu.VMEM((members, NEAR * owned), BF16)],
            aliases={2 + len(halves) + i: i for i in range(len(before))},
        )
        for h, g in zip(halves, gained):
            sums[h] = g
    theirs = move(sums[1], "c", 1)
    (out,) = kernel(
        finish_body,
        [array((members * levels, points), F32)],
        [sums[0], theirs],
        1e8,
        scratch=[pltpu.VMEM((members * levels, points), F32), pltpu.SemaphoreType.DMA((4,))],
        spaces=[None],
    )
    return out.reshape(members, levels, points)


def solution(mesh):
    fine = Mesh(mesh.devices.reshape(16, 4, 4, 2), ("z", "y", "x", "c"))
    tile, level = ("z", "y"), ("x", "c")
    return jax.shard_map(
        shards,
        mesh=fine,
        in_specs=(
            P(None, level, tile),
            P(tile, None),
            P(level, tile),
            P((*tile, *level), None),
            P(),
            P(),
            P(),
            P(tile, None),
        ),
        out_specs=P(None, level, tile),
        check_vma=False,
    )
```

```python
import functools

import jax
import jax.numpy as jnp
from jax import lax
from jax.experimental import pallas as pl
from jax.experimental.pallas import tpu as pltpu
from jax.sharding import Mesh
from jax.sharding import PartitionSpec as P

REACH = 4
NEAR = 6
RELS = 4
F32 = jnp.float32
BF16 = jnp.bfloat16
NT = (((1,), (1,)), ((), ()))
CLASS, CHIP, CORE, COUNT = 6, 12, 13, 14


def kernel(body, out, inputs, flops, scalars=0, scratch=(), aliases=None, given=None, spaces=None):
    spaces = spaces or [pltpu.VMEM] * len(out)
    given = given or [pltpu.SMEM] * scalars + [pltpu.VMEM] * (len(inputs) - scalars)
    inputs = [pltpu.with_memory_space_constraint(a, m) for a, m in zip(inputs, given)]
    return pl.pallas_call(
        body,
        out_shape=[o if m is None else m(o.shape, o.dtype) for o, m in zip(out, spaces)],
        in_specs=[pl.BlockSpec(memory_space=m) for m in given],
        out_specs=[pl.BlockSpec(memory_space=m or pl.ANY) for m in spaces],
        scratch_shapes=list(scratch),
        input_output_aliases=aliases or {},
        cost_estimate=pl.CostEstimate(flops=int(flops), bytes_accessed=int(1e6), transcendentals=0),
        compiler_params=pltpu.CompilerParams(vmem_limit_bytes=16 << 20),
    )(*inputs)


def array(shape, kind):
    return jax.ShapeDtypeStruct(shape, kind)


def move(value, axis, steps):
    count = lax.axis_size(axis)
    return lax.ppermute(value, axis, [(i, (i + steps) % count) for i in range(count)])


def pack_body(*refs):
    given, (meta, out, weights, foot, duals), held = refs[:7], refs[7:12], refs[12:]
    near, count, classes, raw, wide, done = held
    copies = []
    for q, kept in enumerate((near, count, classes, raw, weights, foot, duals)):
        copies.append(pltpu.make_async_copy(given[q], kept, done.at[q]))
    for q in (3, 4, 0, 1, 2, 5, 6):
        copies[q].start()
    copies[3].wait()
    members = out.shape[0] - 16
    levels, slots = weights.shape
    points = raw.shape[1]
    wide[...] = raw[...].astype(F32)
    for l in range(levels):
        plane = wide[pl.ds(l, members, stride=levels), :].astype(BF16)
        out[:members, l * points : (l + 1) * points] = plane
    for q in (4, 0, 1, 2, 5, 6):
        copies[q].wait()
    high = weights[...].astype(BF16).astype(F32)
    low = weights[...] - high
    pad = jnp.zeros((16 - 2 * levels, slots), F32)
    out[members:, :] = jnp.concatenate([high, low, pad], axis=0).astype(BF16)
    tile = lax.axis_index("z") * lax.axis_size("y") + lax.axis_index("y")
    tiles = lax.axis_size("z") * lax.axis_size("y")
    for k in range(NEAR):
        meta[k] = lax.rem(near[k, tile] - tile + REACH + tiles, tiles)
        meta[CLASS + k] = classes[0, k]
    meta[CHIP] = lax.axis_index("x")
    meta[CORE] = lax.axis_index("c")
    meta[COUNT] = count[tile]


def columns(meta, weights, owned):
    parts = []
    for chip in range(RELS):
        block = weights(slice(chip * 2 * owned, (chip + 1) * 2 * owned))
        flipped = jnp.concatenate([block, block], axis=0).T
        parts.append(jnp.where(meta[CORE] == 0, flipped[:owned], flipped[owned:]))
    return jnp.concatenate(parts, axis=0)


def rows_of(meta, foot, owned):
    parts = []
    for chip in range(RELS):
        start = pl.multiple_of(chip * 2 * owned + meta[CORE] * owned, owned)
        parts.append(foot[pl.ds(start, owned), :])
    return jnp.concatenate(parts, axis=0)


def project(picked, column, cells, acc, fresh):
    members = acc.shape[1]
    points = picked.shape[1]
    for l in range(cells.shape[1] // points):
        plane = cells[:members, l * points : (l + 1) * points]
        got = lax.dot_general(picked, plane, NT, preferred_element_type=F32)
        term = column[:, l : l + 1] * got
        if l == 0 and fresh:
            acc[...] = term
        else:
            acc[...] += term


def own_body(meta, foot, cells, weights, out):
    owned = out.shape[0] // RELS
    column = columns(meta, lambda at: weights[:, at], owned)
    project(rows_of(meta, foot, owned), column, cells, out, True)


def other_body(meta, foot, cells, before, duals, pay, acc):
    members = acc.shape[1]
    owned = acc.shape[0] // RELS

    def weights(at):
        terms = cells[members:, at].astype(F32)
        return terms[:4] + terms[4:8]

    acc[...] = before[...]
    project(rows_of(meta, foot, owned), columns(meta, weights, owned), cells, acc, False)
    slot = lax.broadcasted_iota(jnp.int32, (owned, members), 0) + meta[CORE] * owned
    for chip in range(RELS):
        present = slot + chip * 2 * owned < meta[COUNT]
        part = jnp.where(present, acc[chip * owned : (chip + 1) * owned], 0.0)
        high = part.astype(BF16)
        pay[chip, :owned] = high
        pay[chip, owned : 2 * owned] = (part - high.astype(F32)).astype(BF16)
        pay[chip, 2 * owned :] = duals[...]


def fold_body(got, out):
    owned = got.shape[1] // 3
    total = got[0, :owned].astype(F32) + got[0, owned : 2 * owned].astype(F32)
    for chip in range(1, RELS):
        total = total + (got[chip, :owned].astype(F32) + got[chip, owned : 2 * owned].astype(F32))
    out[:owned] = total.astype(BF16)
    for chip in range(RELS):
        out[(chip + 1) * owned : (chip + 2) * owned] = got[chip, 2 * owned :]


def choose(meta, k, sources, size, first, length, store):
    group = meta[k] // 3
    start = pl.multiple_of(lax.rem(meta[k], 3) * size + first, length)
    for g, source in enumerate(sources):

        @pl.when(group == g)
        def _(source=source):
            store(source[pl.ds(start, length), :])


def pick_body(meta, low, mid, high, out):
    size = out.shape[0] // NEAR
    for k in range(NEAR):

        def store(value, k=k):
            out[k * size : (k + 1) * size] = value

        choose(meta, k, (low, mid, high), size, 0, size, store)


def flip_body(meta, low, mid, high, out, held):
    size = held.shape[0] // NEAR
    for r in range(RELS):
        chip = lax.rem(meta[CHIP] + r, RELS)
        for k in range(NEAR):

            def store(value, k=k):
                held[k * size : (k + 1) * size] = value

            choose(meta, k, (low, mid, high), RELS * size, chip * size, size, store)
        out[:, r * held.shape[0] : (r + 1) * held.shape[0]] = held[...].T


def taper_body(meta, taper, out, tall):
    classes = taper.shape[0]
    owned = out.shape[1] // NEAR
    for q in range(classes):
        tall[q] = taper[q].astype(F32).T / F32(511)
    for r in range(RELS):
        chip = lax.rem(meta[CHIP] + r, RELS)
        start = pl.multiple_of(chip * 2 * owned + meta[CORE] * owned, owned)
        for k in range(NEAR):
            out[r, k * owned : (k + 1) * owned] = tall[meta[CLASS + k], pl.ds(start, owned), :]


def covary_body(rel, rows, own, other, scaled, *refs):
    out = refs[-1]
    members = rows.shape[1]
    size = rows.shape[0]
    half = own.shape[1]
    step = 256
    taper = scaled[rel]
    wide = jnp.concatenate([taper] * (step // taper.shape[1]), axis=1)
    for h, cells in enumerate((own, other)):
        for at in range(0, half, step):
            covar = jnp.dot(rows[...], cells[:members, at : at + step], preferred_element_type=F32)
            tapered = (covar * wide).astype(BF16)
            out[rel * size : (rel + 1) * size, h * half + at : h * half + at + step] = tapered


def gain_body(h, duals, tapered, out):
    half = out.shape[1]
    step = 256
    for at in range(0, half, step):
        out[:, at : at + step] = jnp.dot(
            duals[...], tapered[:, h * half + at : h * half + at + step], preferred_element_type=F32
        )


def finish_body(mine, theirs, out, held, done):
    members = mine.shape[0]
    levels = out.shape[0] // members
    points = out.shape[1]
    parts = done.shape[0]
    size = members // parts
    copies = []
    for q in range(parts):
        for l in range(levels):
            at = (slice(q * size, (q + 1) * size), slice(l * points, (l + 1) * points))
            held[pl.ds(q * size * levels + l, size, stride=levels), :] = mine[at] + theirs[at]
        span = pl.ds(q * size * levels, size * levels)
        copies.append(pltpu.make_async_copy(held.at[span], out.at[span], done.at[q]))
        copies[-1].start()
    for copy in copies:
        copy.wait()


def shards(
    anomalies, footprint, weighting, dual_rows, taper_blocks, obs_count, near_tiles, taper_class
):
    members, levels, points = anomalies.shape
    owned = dual_rows.shape[0]
    tile = ("z", "y")
    raw = anomalies.reshape(members * levels, points)
    meta, own, weights, foot, duals = kernel(
        pack_body,
        [
            array((16,), jnp.int32),
            array((members + 16, levels * points), BF16),
            array(weighting.shape, F32),
            array(footprint.shape, BF16),
            array(dual_rows.shape, BF16),
        ],
        [near_tiles.T, obs_count, taper_class, raw, weighting, footprint, dual_rows],
        1e8,
        scratch=[
            pltpu.SMEM(near_tiles.T.shape, jnp.int32),
            pltpu.SMEM(obs_count.shape, jnp.int32),
            pltpu.SMEM(taper_class.shape, jnp.int32),
            pltpu.VMEM(raw.shape, BF16),
            pltpu.VMEM(raw.shape, F32),
            pltpu.SemaphoreType.DMA((7,)),
        ],
        given=[pltpu.HBM] * 7,
        spaces=[pltpu.SMEM] + [pltpu.VMEM] * 4,
    )
    other = move(own, "c", 1)

    rows = RELS * owned
    work = 2 * rows * points * members * levels
    (begun,) = kernel(
        own_body, [array((rows, members), F32)], [meta, foot, own, weights], work, scalars=1
    )
    (pay,) = kernel(
        other_body,
        [array((RELS, 3 * owned, members), BF16)],
        [meta, foot, other, begun, duals],
        work,
        scalars=1,
        scratch=[pltpu.VMEM((rows, members), F32)],
    )
    got = lax.all_to_all(pay, "x", 0, 0, tiled=True)
    (here,) = kernel(fold_body, [array((owned + rows, members), BF16)], [got], 1e8)
    low, high = move(here, tile, 1), move(here, tile, -1)
    y_mid = jnp.concatenate([a[:owned] for a in (low, here, high)], axis=0)
    y_low, y_high = move(y_mid, tile, 3), move(y_mid, tile, -3)
    w_mid = jnp.concatenate([a[owned:] for a in (low, here, high)], axis=0)
    w_low, w_high = move(w_mid, tile, 3), move(w_mid, tile, -3)
    (y0,) = kernel(
        pick_body,
        [array((NEAR * owned, members), BF16)],
        [meta, y_low, y_mid, y_high],
        1e8,
        scalars=1,
    )
    y3, y1, y2 = move(y0, "x", 1), move(y0, "x", -1), move(y0, "x", 2)

    taper_late, _ = lax.optimization_barrier((taper_blocks, y0))
    (scaled,) = kernel(
        taper_body,
        [array((RELS, NEAR * owned, points), F32)],
        [meta, taper_late],
        1e9,
        scalars=1,
        scratch=[pltpu.VMEM((taper_blocks.shape[0], taper_blocks.shape[2], points), F32)],
    )
    width = levels * points
    tapered = None
    for rel, got in ((0, y0), (3, y3), (1, y1), (2, y2)):
        inputs = [got, own, other, scaled] + ([] if tapered is None else [tapered])
        (tapered,) = kernel(
            functools.partial(covary_body, rel),
            [array((NEAR * rows, 2 * width), BF16)],
            inputs,
            4 * NEAR * owned * members * width,
            aliases={} if tapered is None else {4: 0},
        )
    (flipped,) = kernel(
        flip_body,
        [array((members, NEAR * rows), BF16)],
        [meta, w_low, w_mid, w_high],
        1e9,
        scalars=1,
        scratch=[pltpu.VMEM((NEAR * owned, members), BF16)],
    )
    sums = [
        kernel(
            functools.partial(gain_body, h),
            [array((members, width), F32)],
            [flipped, tapered],
            2 * NEAR * rows * members * width,
        )[0]
        for h in (0, 1)
    ]
    theirs = move(sums[1], "c", 1)
    (out,) = kernel(
        finish_body,
        [array((members * levels, points), F32)],
        [sums[0], theirs],
        1e8,
        scratch=[pltpu.VMEM((members * levels, points), F32), pltpu.SemaphoreType.DMA((4,))],
        spaces=[None],
    )
    return out.reshape(members, levels, points)


def solution(mesh):
    fine = Mesh(mesh.devices.reshape(16, 4, 4, 2), ("z", "y", "x", "c"))
    tile, level = ("z", "y"), ("x", "c")
    return jax.shard_map(
        shards,
        mesh=fine,
        in_specs=(
            P(None, level, tile),
            P(tile, None),
            P(level, tile),
            P((*tile, *level), None),
            P(),
            P(),
            P(),
            P(tile, None),
        ),
        out_specs=P(None, level, tile),
        check_vma=False,
    )
```

```python
import functools

import jax
import jax.numpy as jnp
from jax import lax
from jax.experimental import pallas as pl
from jax.experimental.pallas import tpu as pltpu
from jax.sharding import Mesh
from jax.sharding import PartitionSpec as P

REACH = 4
NEAR = 6
RELS = 4
F32 = jnp.float32
BF16 = jnp.bfloat16
NT = (((1,), (1,)), ((), ()))
CLASS, CHIP, CORE, COUNT = 6, 12, 13, 14


def kernel(body, out, inputs, flops, scalars=0, scratch=(), aliases=None, given=None, spaces=None):
    spaces = spaces or [pltpu.VMEM] * len(out)
    given = given or [pltpu.SMEM] * scalars + [pltpu.VMEM] * (len(inputs) - scalars)
    inputs = [pltpu.with_memory_space_constraint(a, m) for a, m in zip(inputs, given)]
    return pl.pallas_call(
        body,
        out_shape=[o if m is None else m(o.shape, o.dtype) for o, m in zip(out, spaces)],
        in_specs=[pl.BlockSpec(memory_space=m) for m in given],
        out_specs=[pl.BlockSpec(memory_space=m or pl.ANY) for m in spaces],
        scratch_shapes=list(scratch),
        input_output_aliases=aliases or {},
        cost_estimate=pl.CostEstimate(flops=int(flops), bytes_accessed=int(1e6), transcendentals=0),
        compiler_params=pltpu.CompilerParams(vmem_limit_bytes=16 << 20),
    )(*inputs)


def array(shape, kind):
    return jax.ShapeDtypeStruct(shape, kind)


def move(value, axis, steps):
    count = lax.axis_size(axis)
    return lax.ppermute(value, axis, [(i, (i + steps) % count) for i in range(count)])


def pack_body(*refs):
    given, (meta, out, weights, foot, duals), held = refs[:7], refs[7:12], refs[12:]
    near, count, classes, raw, wide, done = held
    copies = []
    for q, kept in enumerate((near, count, classes, raw, weights, foot, duals)):
        copies.append(pltpu.make_async_copy(given[q], kept, done.at[q]))
    for q in (3, 4, 0, 1, 2, 5, 6):
        copies[q].start()
    copies[3].wait()
    members = out.shape[0] - 16
    levels, slots = weights.shape
    points = raw.shape[1]
    wide[...] = raw[...].astype(F32)
    for l in range(levels):
        plane = wide[pl.ds(l, members, stride=levels), :].astype(BF16)
        out[:members, l * points : (l + 1) * points] = plane
    for q in (4, 0, 1, 2, 5, 6):
        copies[q].wait()
    high = weights[...].astype(BF16).astype(F32)
    low = weights[...] - high
    pad = jnp.zeros((16 - 2 * levels, slots), F32)
    out[members:, :] = jnp.concatenate([high, low, pad], axis=0).astype(BF16)
    tile = lax.axis_index("z") * lax.axis_size("y") + lax.axis_index("y")
    tiles = lax.axis_size("z") * lax.axis_size("y")
    for k in range(NEAR):
        meta[k] = lax.rem(near[k, tile] - tile + REACH + tiles, tiles)
        meta[CLASS + k] = classes[0, k]
    meta[CHIP] = lax.axis_index("x")
    meta[CORE] = lax.axis_index("c")
    meta[COUNT] = count[tile]


def columns(meta, weights, owned):
    parts = []
    for chip in range(RELS):
        block = weights(slice(chip * 2 * owned, (chip + 1) * 2 * owned))
        flipped = jnp.concatenate([block, block], axis=0).T
        parts.append(jnp.where(meta[CORE] == 0, flipped[:owned], flipped[owned:]))
    return jnp.concatenate(parts, axis=0)


def rows_of(meta, foot, owned):
    parts = []
    for chip in range(RELS):
        start = pl.multiple_of(chip * 2 * owned + meta[CORE] * owned, owned)
        parts.append(foot[pl.ds(start, owned), :])
    return jnp.concatenate(parts, axis=0)


def project(picked, column, cells, acc, fresh):
    members = acc.shape[1]
    points = picked.shape[1]
    for l in range(cells.shape[1] // points):
        plane = cells[:members, l * points : (l + 1) * points]
        got = lax.dot_general(picked, plane, NT, preferred_element_type=F32)
        term = column[:, l : l + 1] * got
        if l == 0 and fresh:
            acc[...] = term
        else:
            acc[...] += term


def own_body(meta, foot, cells, weights, out):
    owned = out.shape[0] // RELS
    column = columns(meta, lambda at: weights[:, at], owned)
    project(rows_of(meta, foot, owned), column, cells, out, True)


def other_body(meta, foot, cells, before, duals, pay, acc):
    members = acc.shape[1]
    owned = acc.shape[0] // RELS

    def weights(at):
        terms = cells[members:, at].astype(F32)
        return terms[:4] + terms[4:8]

    acc[...] = before[...]
    project(rows_of(meta, foot, owned), columns(meta, weights, owned), cells, acc, False)
    slot = lax.broadcasted_iota(jnp.int32, (owned, members), 0) + meta[CORE] * owned
    for chip in range(RELS):
        present = slot + chip * 2 * owned < meta[COUNT]
        part = jnp.where(present, acc[chip * owned : (chip + 1) * owned], 0.0)
        high = part.astype(BF16)
        pay[chip, :owned] = high
        pay[chip, owned : 2 * owned] = (part - high.astype(F32)).astype(BF16)
        pay[chip, 2 * owned :] = duals[...]


def fold_body(got, out):
    owned = got.shape[1] // 3
    total = got[0, :owned].astype(F32) + got[0, owned : 2 * owned].astype(F32)
    for chip in range(1, RELS):
        total = total + (got[chip, :owned].astype(F32) + got[chip, owned : 2 * owned].astype(F32))
    out[:owned] = total.astype(BF16)
    for chip in range(RELS):
        out[(chip + 1) * owned : (chip + 2) * owned] = got[chip, 2 * owned :]


def choose(meta, k, sources, size, first, length, store):
    group = meta[k] // 3
    start = pl.multiple_of(lax.rem(meta[k], 3) * size + first, length)
    for g, source in enumerate(sources):

        @pl.when(group == g)
        def _(source=source):
            store(source[pl.ds(start, length), :])


def pick_body(meta, low, mid, high, out):
    size = out.shape[0] // NEAR
    for k in range(NEAR):

        def store(value, k=k):
            out[k * size : (k + 1) * size] = value

        choose(meta, k, (low, mid, high), size, 0, size, store)


def flip_body(meta, low, mid, high, out, held):
    size = held.shape[0] // NEAR
    for r in range(RELS):
        chip = lax.rem(meta[CHIP] + r, RELS)
        for k in range(NEAR):

            def store(value, k=k):
                held[k * size : (k + 1) * size] = value

            choose(meta, k, (low, mid, high), RELS * size, chip * size, size, store)
        out[:, r * held.shape[0] : (r + 1) * held.shape[0]] = held[...].T


def taper_body(meta, taper, out, tall):
    classes = taper.shape[0]
    owned = out.shape[1] // NEAR
    for q in range(classes):
        tall[q] = taper[q].astype(F32).T / F32(511)
    for r in range(RELS):
        chip = lax.rem(meta[CHIP] + r, RELS)
        start = pl.multiple_of(chip * 2 * owned + meta[CORE] * owned, owned)
        for k in range(NEAR):
            out[r, k * owned : (k + 1) * owned] = tall[meta[CLASS + k], pl.ds(start, owned), :]


def covary_body(rel, rows, own, other, scaled, *refs):
    out = refs[-1]
    members = rows.shape[1]
    size = rows.shape[0]
    half = own.shape[1]
    step = 256
    taper = scaled[rel]
    wide = jnp.concatenate([taper] * (step // taper.shape[1]), axis=1)
    for h, cells in enumerate((own, other)):
        for at in range(0, half, step):
            covar = jnp.dot(rows[...], cells[:members, at : at + step], preferred_element_type=F32)
            tapered = (covar * wide).astype(BF16)
            out[rel * size : (rel + 1) * size, h * half + at : h * half + at + step] = tapered


def gain_body(h, duals, tapered, out):
    half = out.shape[1]
    step = 256
    for at in range(0, half, step):
        span = slice(h * half + at, h * half + at + step)
        gained = jnp.dot(duals[...], tapered[:, span], preferred_element_type=F32)
        out[:, at : at + step] = gained.astype(out.dtype)


def finish_body(mine, theirs, out, held, done):
    members = mine.shape[0]
    levels = out.shape[0] // members
    points = out.shape[1]
    parts = done.shape[0]
    size = members // parts
    copies = []
    for q in range(parts):
        for l in range(levels):
            at = (slice(q * size, (q + 1) * size), slice(l * points, (l + 1) * points))
            held[pl.ds(q * size * levels + l, size, stride=levels), :] = mine[at] + theirs[at].astype(F32)
        span = pl.ds(q * size * levels, size * levels)
        copies.append(pltpu.make_async_copy(held.at[span], out.at[span], done.at[q]))
        copies[-1].start()
    for copy in copies:
        copy.wait()


def shards(
    anomalies, footprint, weighting, dual_rows, taper_blocks, obs_count, near_tiles, taper_class
):
    members, levels, points = anomalies.shape
    owned = dual_rows.shape[0]
    tile = ("z", "y")
    raw = anomalies.reshape(members * levels, points)
    meta, own, weights, foot, duals = kernel(
        pack_body,
        [
            array((16,), jnp.int32),
            array((members + 16, levels * points), BF16),
            array(weighting.shape, F32),
            array(footprint.shape, BF16),
            array(dual_rows.shape, BF16),
        ],
        [near_tiles.T, obs_count, taper_class, raw, weighting, footprint, dual_rows],
        1e8,
        scratch=[
            pltpu.SMEM(near_tiles.T.shape, jnp.int32),
            pltpu.SMEM(obs_count.shape, jnp.int32),
            pltpu.SMEM(taper_class.shape, jnp.int32),
            pltpu.VMEM(raw.shape, BF16),
            pltpu.VMEM(raw.shape, F32),
            pltpu.SemaphoreType.DMA((7,)),
        ],
        given=[pltpu.HBM] * 7,
        spaces=[pltpu.SMEM] + [pltpu.VMEM] * 4,
    )
    other = move(own, "c", 1)

    rows = RELS * owned
    work = 2 * rows * points * members * levels
    (begun,) = kernel(
        own_body, [array((rows, members), F32)], [meta, foot, own, weights], work, scalars=1
    )
    (pay,) = kernel(
        other_body,
        [array((RELS, 3 * owned, members), BF16)],
        [meta, foot, other, begun, duals],
        work,
        scalars=1,
        scratch=[pltpu.VMEM((rows, members), F32)],
    )
    got = lax.all_to_all(pay, "x", 0, 0, tiled=True)
    (here,) = kernel(fold_body, [array((owned + rows, members), BF16)], [got], 1e8)
    low, high = move(here, tile, 1), move(here, tile, -1)
    y_mid = jnp.concatenate([a[:owned] for a in (low, here, high)], axis=0)
    y_low, y_high = move(y_mid, tile, 3), move(y_mid, tile, -3)
    w_mid = jnp.concatenate([a[owned:] for a in (low, here, high)], axis=0)
    w_low, w_high = move(w_mid, tile, 3), move(w_mid, tile, -3)
    (y0,) = kernel(
        pick_body,
        [array((NEAR * owned, members), BF16)],
        [meta, y_low, y_mid, y_high],
        1e8,
        scalars=1,
    )
    y3, y1, y2 = move(y0, "x", 1), move(y0, "x", -1), move(y0, "x", 2)

    taper_late, _ = lax.optimization_barrier((taper_blocks, y0))
    (scaled,) = kernel(
        taper_body,
        [array((RELS, NEAR * owned, points), F32)],
        [meta, taper_late],
        1e9,
        scalars=1,
        scratch=[pltpu.VMEM((taper_blocks.shape[0], taper_blocks.shape[2], points), F32)],
    )
    width = levels * points
    (flipped,) = kernel(
        flip_body,
        [array((members, NEAR * rows), BF16)],
        [meta, w_low, w_mid, w_high],
        1e9,
        scalars=1,
        scratch=[pltpu.VMEM((NEAR * owned, members), BF16)],
    )
    y3, y1, y2 = (lax.optimization_barrier((y, flipped))[0] for y in (y3, y1, y2))
    tapered = None
    for rel, got in ((0, y0), (2, y2), (3, y3), (1, y1)):
        inputs = [got, own, other, scaled] + ([] if tapered is None else [tapered])
        (tapered,) = kernel(
            functools.partial(covary_body, rel),
            [array((NEAR * rows, 2 * width), BF16)],
            inputs,
            4 * NEAR * owned * members * width,
            aliases={} if tapered is None else {4: 0},
        )
    sums = [
        kernel(
            functools.partial(gain_body, h),
            [array((members, width), BF16 if h else F32)],
            [flipped, tapered],
            2 * NEAR * rows * members * width,
        )[0]
        for h in (0, 1)
    ]
    theirs = move(sums[1], "c", 1)
    (out,) = kernel(
        finish_body,
        [array((members * levels, points), F32)],
        [sums[0], theirs],
        1e8,
        scratch=[pltpu.VMEM((members * levels, points), F32), pltpu.SemaphoreType.DMA((4,))],
        spaces=[None],
    )
    return out.reshape(members, levels, points)


def solution(mesh):
    fine = Mesh(mesh.devices.reshape(16, 4, 4, 2), ("z", "y", "x", "c"))
    tile, level = ("z", "y"), ("x", "c")
    return jax.shard_map(
        shards,
        mesh=fine,
        in_specs=(
            P(None, level, tile),
            P(tile, None),
            P(level, tile),
            P((*tile, *level), None),
            P(),
            P(),
            P(),
            P(tile, None),
        ),
        out_specs=P(None, level, tile),
        check_vma=False,
    )
```

```python
import functools

import jax
import jax.numpy as jnp
from jax import lax
from jax.experimental import pallas as pl
from jax.experimental.pallas import tpu as pltpu
from jax.sharding import Mesh
from jax.sharding import PartitionSpec as P

REACH = 4
NEAR = 6
RELS = 4
F32 = jnp.float32
BF16 = jnp.bfloat16
NT = (((1,), (1,)), ((), ()))
CLASS, CHIP, CORE, COUNT = 6, 12, 13, 14


def kernel(body, out, inputs, flops, scalars=0, scratch=(), aliases=None, given=None, spaces=None):
    spaces = spaces or [pltpu.VMEM] * len(out)
    given = given or [pltpu.SMEM] * scalars + [pltpu.VMEM] * (len(inputs) - scalars)
    inputs = [pltpu.with_memory_space_constraint(a, m) for a, m in zip(inputs, given)]
    return pl.pallas_call(
        body,
        out_shape=[o if m is None else m(o.shape, o.dtype) for o, m in zip(out, spaces)],
        in_specs=[pl.BlockSpec(memory_space=m) for m in given],
        out_specs=[pl.BlockSpec(memory_space=m or pl.ANY) for m in spaces],
        scratch_shapes=list(scratch),
        input_output_aliases=aliases or {},
        cost_estimate=pl.CostEstimate(flops=int(flops), bytes_accessed=int(1e6), transcendentals=0),
        compiler_params=pltpu.CompilerParams(vmem_limit_bytes=16 << 20),
    )(*inputs)


def array(shape, kind):
    return jax.ShapeDtypeStruct(shape, kind)


def move(value, axis, steps):
    count = lax.axis_size(axis)
    return lax.ppermute(value, axis, [(i, (i + steps) % count) for i in range(count)])


def pack_body(*refs):
    given, (meta, out, weights, foot, duals), held = refs[:7], refs[7:12], refs[12:]
    near, count, classes, raw, wide, done = held
    copies = []
    for q, kept in enumerate((near, count, classes, raw, weights, foot, duals)):
        copies.append(pltpu.make_async_copy(given[q], kept, done.at[q]))
    for q in (3, 4, 0, 1, 2, 5, 6):
        copies[q].start()
    copies[3].wait()
    members = out.shape[0] - 16
    levels, slots = weights.shape
    points = raw.shape[1]
    wide[...] = raw[...].astype(F32)
    for l in range(levels):
        plane = wide[pl.ds(l, members, stride=levels), :].astype(BF16)
        out[:members, l * points : (l + 1) * points] = plane
    for q in (4, 0, 1, 2, 5, 6):
        copies[q].wait()
    high = weights[...].astype(BF16).astype(F32)
    low = weights[...] - high
    pad = jnp.zeros((16 - 2 * levels, slots), F32)
    out[members:, :] = jnp.concatenate([high, low, pad], axis=0).astype(BF16)
    tile = lax.axis_index("z") * lax.axis_size("y") + lax.axis_index("y")
    tiles = lax.axis_size("z") * lax.axis_size("y")
    for k in range(NEAR):
        meta[k] = lax.rem(near[k, tile] - tile + REACH + tiles, tiles)
        meta[CLASS + k] = classes[0, k]
    meta[CHIP] = lax.axis_index("x")
    meta[CORE] = lax.axis_index("c")
    meta[COUNT] = count[tile]


def columns(meta, weights, owned):
    parts = []
    for chip in range(RELS):
        block = weights(slice(chip * 2 * owned, (chip + 1) * 2 * owned))
        flipped = jnp.concatenate([block, block], axis=0).T
        parts.append(jnp.where(meta[CORE] == 0, flipped[:owned], flipped[owned:]))
    return jnp.concatenate(parts, axis=0)


def rows_of(meta, foot, owned):
    parts = []
    for chip in range(RELS):
        start = pl.multiple_of(chip * 2 * owned + meta[CORE] * owned, owned)
        parts.append(foot[pl.ds(start, owned), :])
    return jnp.concatenate(parts, axis=0)


def project(picked, column, cells, acc, fresh):
    members = acc.shape[1]
    points = picked.shape[1]
    for l in range(cells.shape[1] // points):
        plane = cells[:members, l * points : (l + 1) * points]
        got = lax.dot_general(picked, plane, NT, preferred_element_type=F32)
        term = column[:, l : l + 1] * got
        if l == 0 and fresh:
            acc[...] = term
        else:
            acc[...] += term


def own_body(meta, foot, cells, weights, out):
    owned = out.shape[0] // RELS
    column = columns(meta, lambda at: weights[:, at], owned)
    project(rows_of(meta, foot, owned), column, cells, out, True)


def other_body(meta, foot, cells, before, duals, pay, acc):
    members = acc.shape[1]
    owned = acc.shape[0] // RELS

    def weights(at):
        terms = cells[members:, at].astype(F32)
        return terms[:4] + terms[4:8]

    acc[...] = before[...]
    project(rows_of(meta, foot, owned), columns(meta, weights, owned), cells, acc, False)
    slot = lax.broadcasted_iota(jnp.int32, (owned, members), 0) + meta[CORE] * owned
    for chip in range(RELS):
        present = slot + chip * 2 * owned < meta[COUNT]
        part = jnp.where(present, acc[chip * owned : (chip + 1) * owned], 0.0)
        high = part.astype(BF16)
        pay[chip, :owned] = high
        pay[chip, owned : 2 * owned] = (part - high.astype(F32)).astype(BF16)
        pay[chip, 2 * owned :] = duals[...]


def fold_body(got, out):
    owned = got.shape[1] // 3
    total = got[0, :owned].astype(F32) + got[0, owned : 2 * owned].astype(F32)
    for chip in range(1, RELS):
        total = total + (got[chip, :owned].astype(F32) + got[chip, owned : 2 * owned].astype(F32))
    out[:owned] = total.astype(BF16)
    for chip in range(RELS):
        out[(chip + 1) * owned : (chip + 2) * owned] = got[chip, 2 * owned :]


def choose(meta, k, sources, size, first, length, store):
    group = meta[k] // 3
    start = pl.multiple_of(lax.rem(meta[k], 3) * size + first, length)
    for g, source in enumerate(sources):

        @pl.when(group == g)
        def _(source=source):
            store(source[pl.ds(start, length), :])


def pick_body(meta, low, mid, high, out):
    size = out.shape[0] // NEAR
    for k in range(NEAR):

        def store(value, k=k):
            out[k * size : (k + 1) * size] = value

        choose(meta, k, (low, mid, high), size, 0, size, store)


def flip_body(meta, low, mid, high, out, held):
    size = held.shape[0] // NEAR
    for r in range(RELS):
        chip = lax.rem(meta[CHIP] + r, RELS)
        for k in range(NEAR):

            def store(value, k=k):
                held[k * size : (k + 1) * size] = value

            choose(meta, k, (low, mid, high), RELS * size, chip * size, size, store)
        out[:, r * held.shape[0] : (r + 1) * held.shape[0]] = held[...].T


def taper_body(meta, taper, out, tall):
    classes = taper.shape[0]
    owned = out.shape[1] // NEAR
    for q in range(classes):
        tall[q] = taper[q].astype(F32).T / F32(511)
    for r in range(RELS):
        chip = lax.rem(meta[CHIP] + r, RELS)
        start = pl.multiple_of(chip * 2 * owned + meta[CORE] * owned, owned)
        for k in range(NEAR):
            out[r, k * owned : (k + 1) * owned] = tall[meta[CLASS + k], pl.ds(start, owned), :]


def analyse_body(rels, count, *refs):
    rows, (scaled, flipped) = refs[: len(rels)], refs[len(rels) : len(rels) + 2]
    cells = refs[len(rels) + 2 : len(rels) + 2 + count]
    before, outs = refs[len(rels) + 2 + count : -count], refs[-count:]
    size, members = rows[0].shape
    step = 256
    for h in range(count):
        for at in range(0, outs[h].shape[1], step):
            span = slice(at, at + step)
            total = before[h][:, span] if before else None
            for rel, got in zip(rels, rows):
                taper = scaled[rel]
                wide = jnp.concatenate([taper] * (step // taper.shape[1]), axis=1)
                covar = jnp.dot(got[...], cells[h][:members, span], preferred_element_type=F32)
                tapered = (covar * wide).astype(BF16)
                duals = flipped[:, rel * size : (rel + 1) * size]
                gained = jnp.dot(duals, tapered, preferred_element_type=F32)
                total = gained if total is None else total + gained
            outs[h][:, span] = total.astype(outs[h].dtype)


def finish_body(mine, theirs, out, held, done):
    members = mine.shape[0]
    levels = out.shape[0] // members
    points = out.shape[1]
    parts = done.shape[0]
    size = members // parts
    copies = []
    for q in range(parts):
        for l in range(levels):
            at = (slice(q * size, (q + 1) * size), slice(l * points, (l + 1) * points))
            held[pl.ds(q * size * levels + l, size, stride=levels), :] = mine[at] + theirs[at].astype(F32)
        span = pl.ds(q * size * levels, size * levels)
        copies.append(pltpu.make_async_copy(held.at[span], out.at[span], done.at[q]))
        copies[-1].start()
    for copy in copies:
        copy.wait()


def shards(
    anomalies, footprint, weighting, dual_rows, taper_blocks, obs_count, near_tiles, taper_class
):
    members, levels, points = anomalies.shape
    owned = dual_rows.shape[0]
    tile = ("z", "y")
    raw = anomalies.reshape(members * levels, points)
    meta, own, weights, foot, duals = kernel(
        pack_body,
        [
            array((16,), jnp.int32),
            array((members + 16, levels * points), BF16),
            array(weighting.shape, F32),
            array(footprint.shape, BF16),
            array(dual_rows.shape, BF16),
        ],
        [near_tiles.T, obs_count, taper_class, raw, weighting, footprint, dual_rows],
        1e8,
        scratch=[
            pltpu.SMEM(near_tiles.T.shape, jnp.int32),
            pltpu.SMEM(obs_count.shape, jnp.int32),
            pltpu.SMEM(taper_class.shape, jnp.int32),
            pltpu.VMEM(raw.shape, BF16),
            pltpu.VMEM(raw.shape, F32),
            pltpu.SemaphoreType.DMA((7,)),
        ],
        given=[pltpu.HBM] * 7,
        spaces=[pltpu.SMEM] + [pltpu.VMEM] * 4,
    )
    other = move(own, "c", 1)

    rows = RELS * owned
    work = 2 * rows * points * members * levels
    (begun,) = kernel(
        own_body, [array((rows, members), F32)], [meta, foot, own, weights], work, scalars=1
    )
    (pay,) = kernel(
        other_body,
        [array((RELS, 3 * owned, members), BF16)],
        [meta, foot, other, begun, duals],
        work,
        scalars=1,
        scratch=[pltpu.VMEM((rows, members), F32)],
    )
    got = lax.all_to_all(pay, "x", 0, 0, tiled=True)
    (here,) = kernel(fold_body, [array((owned + rows, members), BF16)], [got], 1e8)
    low, high = move(here, tile, 1), move(here, tile, -1)
    y_mid = jnp.concatenate([a[:owned] for a in (low, here, high)], axis=0)
    y_low, y_high = move(y_mid, tile, 3), move(y_mid, tile, -3)
    w_mid = jnp.concatenate([a[owned:] for a in (low, here, high)], axis=0)
    w_low, w_high = move(w_mid, tile, 3), move(w_mid, tile, -3)
    (y0,) = kernel(
        pick_body,
        [array((NEAR * owned, members), BF16)],
        [meta, y_low, y_mid, y_high],
        1e8,
        scalars=1,
    )
    y3, y1, y2 = move(y0, "x", 1), move(y0, "x", -1), move(y0, "x", 2)

    taper_late, _ = lax.optimization_barrier((taper_blocks, y0))
    (scaled,) = kernel(
        taper_body,
        [array((RELS, NEAR * owned, points), F32)],
        [meta, taper_late],
        1e9,
        scalars=1,
        scratch=[pltpu.VMEM((taper_blocks.shape[0], taper_blocks.shape[2], points), F32)],
    )
    width = levels * points
    (flipped,) = kernel(
        flip_body,
        [array((members, NEAR * rows), BF16)],
        [meta, w_low, w_mid, w_high],
        1e9,
        scalars=1,
        scratch=[pltpu.VMEM((NEAR * owned, members), BF16)],
    )

    def analyse(rels, rows, halves, before, kind):
        planes = [(own, other)[h] for h in halves]
        return kernel(
            functools.partial(analyse_body, rels, len(halves)),
            [array((members, width), kind)] * len(halves),
            [*rows, scaled, flipped, *planes, *before],
            4 * NEAR * owned * members * width * len(halves) * len(rels),
        )

    sums = analyse((0,), (y0,), (0, 1), (), F32)
    sums = analyse((2,), (y2,), (0, 1), sums, F32)
    (given,) = analyse((3, 1), (y3, y1), (1,), sums[1:], BF16)
    (kept,) = analyse((3, 1), (y3, y1), (0,), sums[:1], F32)
    theirs = move(given, "c", 1)
    (out,) = kernel(
        finish_body,
        [array((members * levels, points), F32)],
        [kept, theirs],
        1e8,
        scratch=[pltpu.VMEM((members * levels, points), F32), pltpu.SemaphoreType.DMA((4,))],
        spaces=[None],
    )
    return out.reshape(members, levels, points)


def solution(mesh):
    fine = Mesh(mesh.devices.reshape(16, 4, 4, 2), ("z", "y", "x", "c"))
    tile, level = ("z", "y"), ("x", "c")
    return jax.shard_map(
        shards,
        mesh=fine,
        in_specs=(
            P(None, level, tile),
            P(tile, None),
            P(level, tile),
            P((*tile, *level), None),
            P(),
            P(),
            P(),
            P(tile, None),
        ),
        out_specs=P(None, level, tile),
        check_vma=False,
    )
```

```python
import functools

import jax
import jax.numpy as jnp
from jax import lax
from jax.experimental import pallas as pl
from jax.experimental.pallas import tpu as pltpu
from jax.sharding import Mesh
from jax.sharding import PartitionSpec as P

REACH = 4
NEAR = 6
RELS = 4
TURNS = (0, 2, 3, 1)
F32 = jnp.float32
BF16 = jnp.bfloat16
NT = (((1,), (1,)), ((), ()))
CLASS, CHIP, CORE, COUNT = 6, 12, 13, 14


def kernel(body, out, inputs, flops, scalars=0, scratch=(), aliases=None, given=None, spaces=None):
    spaces = spaces or [pltpu.VMEM] * len(out)
    given = given or [pltpu.SMEM] * scalars + [pltpu.VMEM] * (len(inputs) - scalars)
    inputs = [pltpu.with_memory_space_constraint(a, m) for a, m in zip(inputs, given)]
    return pl.pallas_call(
        body,
        out_shape=[o if m is None else m(o.shape, o.dtype) for o, m in zip(out, spaces)],
        in_specs=[pl.BlockSpec(memory_space=m) for m in given],
        out_specs=[pl.BlockSpec(memory_space=m or pl.ANY) for m in spaces],
        scratch_shapes=list(scratch),
        input_output_aliases=aliases or {},
        cost_estimate=pl.CostEstimate(flops=int(flops), bytes_accessed=int(1e6), transcendentals=0),
        compiler_params=pltpu.CompilerParams(vmem_limit_bytes=16 << 20),
    )(*inputs)


def array(shape, kind):
    return jax.ShapeDtypeStruct(shape, kind)


def move(value, axis, steps):
    count = lax.axis_size(axis)
    return lax.ppermute(value, axis, [(i, (i + steps) % count) for i in range(count)])


def pack_body(*refs):
    given, (meta, out, weights, foot, duals), held = refs[:7], refs[7:12], refs[12:]
    near, count, classes, raw, wide, done = held
    copies = []
    for q, kept in enumerate((near, count, classes, raw, weights, foot, duals)):
        copies.append(pltpu.make_async_copy(given[q], kept, done.at[q]))
    for q in (3, 4, 0, 1, 2, 5, 6):
        copies[q].start()
    copies[3].wait()
    members = out.shape[0] - 16
    levels, slots = weights.shape
    points = raw.shape[1]
    wide[...] = raw[...].astype(F32)
    for l in range(levels):
        plane = wide[pl.ds(l, members, stride=levels), :].astype(BF16)
        out[:members, l * points : (l + 1) * points] = plane
    for q in (4, 0, 1, 2, 5, 6):
        copies[q].wait()
    high = weights[...].astype(BF16).astype(F32)
    low = weights[...] - high
    pad = jnp.zeros((16 - 2 * levels, slots), F32)
    out[members:, :] = jnp.concatenate([high, low, pad], axis=0).astype(BF16)
    tile = lax.axis_index("z") * lax.axis_size("y") + lax.axis_index("y")
    tiles = lax.axis_size("z") * lax.axis_size("y")
    for k in range(NEAR):
        meta[k] = lax.rem(near[k, tile] - tile + REACH + tiles, tiles)
        meta[CLASS + k] = classes[0, k]
    meta[CHIP] = lax.axis_index("x")
    meta[CORE] = lax.axis_index("c")
    meta[COUNT] = count[tile]


def columns(meta, weights, owned):
    parts = []
    for chip in range(RELS):
        block = weights(slice(chip * 2 * owned, (chip + 1) * 2 * owned))
        flipped = jnp.concatenate([block, block], axis=0).T
        parts.append(jnp.where(meta[CORE] == 0, flipped[:owned], flipped[owned:]))
    return jnp.concatenate(parts, axis=0)


def rows_of(meta, foot, owned):
    parts = []
    for chip in range(RELS):
        start = pl.multiple_of(chip * 2 * owned + meta[CORE] * owned, owned)
        parts.append(foot[pl.ds(start, owned), :])
    return jnp.concatenate(parts, axis=0)


def project(picked, column, cells, acc, fresh):
    members = acc.shape[1]
    points = picked.shape[1]
    for l in range(cells.shape[1] // points):
        plane = cells[:members, l * points : (l + 1) * points]
        got = lax.dot_general(picked, plane, NT, preferred_element_type=F32)
        term = column[:, l : l + 1] * got
        if l == 0 and fresh:
            acc[...] = term
        else:
            acc[...] += term


def own_body(meta, foot, cells, weights, out):
    owned = out.shape[0] // RELS
    column = columns(meta, lambda at: weights[:, at], owned)
    project(rows_of(meta, foot, owned), column, cells, out, True)


def other_body(meta, foot, cells, before, duals, pay, acc):
    members = acc.shape[1]
    owned = acc.shape[0] // RELS

    def weights(at):
        terms = cells[members:, at].astype(F32)
        return terms[:4] + terms[4:8]

    acc[...] = before[...]
    project(rows_of(meta, foot, owned), columns(meta, weights, owned), cells, acc, False)
    slot = lax.broadcasted_iota(jnp.int32, (owned, members), 0) + meta[CORE] * owned
    for chip in range(RELS):
        present = slot + chip * 2 * owned < meta[COUNT]
        part = jnp.where(present, acc[chip * owned : (chip + 1) * owned], 0.0)
        high = part.astype(BF16)
        pay[chip, :owned] = high
        pay[chip, owned : 2 * owned] = (part - high.astype(F32)).astype(BF16)
        pay[chip, 2 * owned :] = duals[...]


def fold_body(got, out):
    owned = got.shape[1] // 3
    total = got[0, :owned].astype(F32) + got[0, owned : 2 * owned].astype(F32)
    for chip in range(1, RELS):
        total = total + (got[chip, :owned].astype(F32) + got[chip, owned : 2 * owned].astype(F32))
    out[:owned] = total.astype(BF16)
    for chip in range(RELS):
        out[(chip + 1) * owned : (chip + 2) * owned] = got[chip, 2 * owned :]


def choose(meta, k, sources, size, first, length, store):
    group = meta[k] // 3
    start = pl.multiple_of(lax.rem(meta[k], 3) * size + first, length)
    for g, source in enumerate(sources):

        @pl.when(group == g)
        def _(source=source):
            store(source[pl.ds(start, length), :])


def pick_body(meta, low, mid, high, out):
    size = out.shape[0] // NEAR
    for k in range(NEAR):

        def store(value, k=k):
            out[k * size : (k + 1) * size] = value

        choose(meta, k, (low, mid, high), size, 0, size, store)


def flip_body(meta, low, mid, high, out, held):
    size = held.shape[0] // NEAR
    for r, turn in enumerate(TURNS):
        chip = lax.rem(meta[CHIP] + turn, RELS)
        for k in range(NEAR):

            def store(value, k=k):
                held[k * size : (k + 1) * size] = value

            choose(meta, k, (low, mid, high), RELS * size, chip * size, size, store)
        out[:, r * held.shape[0] : (r + 1) * held.shape[0]] = held[...].T


def taper_body(meta, taper, out, tall):
    classes = taper.shape[0]
    owned = out.shape[1] // NEAR
    for q in range(classes):
        tall[q] = taper[q].astype(F32).T / F32(511)
    for r in range(RELS):
        chip = lax.rem(meta[CHIP] + r, RELS)
        start = pl.multiple_of(chip * 2 * owned + meta[CORE] * owned, owned)
        for k in range(NEAR):
            out[r, k * owned : (k + 1) * owned] = tall[meta[CLASS + k], pl.ds(start, owned), :]


def covariance(rows, cells, scaled, span):
    members = rows.shape[1]
    taper = scaled[...]
    wide = jnp.concatenate([taper] * ((span.stop - span.start) // taper.shape[1]), axis=1)
    covar = jnp.dot(rows[...], cells[:members, span], preferred_element_type=F32)
    return (covar * wide).astype(BF16)


def covary_body(place, rows, own, other, scaled, *refs):
    out = refs[-1]
    size = rows.shape[0]
    half = own.shape[1]
    for h, cells in enumerate((own, other)):
        for at in range(0, half, 256):
            got = covariance(rows, cells, scaled.at[TURNS[place]], slice(at, at + 256))
            first = h * half + at
            out[place * size : (place + 1) * size, first : first + 256] = got


def gain_body(flipped, tapered, *outs):
    depth = tapered.shape[0]
    half = outs[0].shape[1]
    for h, out in enumerate(outs):
        for at in range(0, half, 256):
            block = tapered[:, h * half + at : h * half + at + 256]
            out[:, at : at + 256] = jnp.dot(flipped[:, :depth], block, preferred_element_type=F32)


def late_body(rows3, rows1, scaled, flipped, cells, before, out):
    depth = 2 * rows3.shape[0]
    for at in range(0, out.shape[1], 256):
        span = slice(at, at + 256)
        parts = [covariance(y, cells, scaled.at[r], span) for r, y in ((3, rows3), (1, rows1))]
        both = jnp.concatenate(parts, axis=0)
        gained = jnp.dot(flipped[:, depth:], both, preferred_element_type=F32)
        out[:, span] = (before[:, span] + gained).astype(out.dtype)


def finish_body(mine, theirs, out, held, done):
    members = mine.shape[0]
    levels = out.shape[0] // members
    points = out.shape[1]
    parts = done.shape[0]
    size = members // parts
    copies = []
    for q in range(parts):
        for l in range(levels):
            at = (slice(q * size, (q + 1) * size), slice(l * points, (l + 1) * points))
            held[pl.ds(q * size * levels + l, size, stride=levels), :] = mine[at] + theirs[at].astype(F32)
        span = pl.ds(q * size * levels, size * levels)
        copies.append(pltpu.make_async_copy(held.at[span], out.at[span], done.at[q]))
        copies[-1].start()
    for copy in copies:
        copy.wait()


def shards(
    anomalies, footprint, weighting, dual_rows, taper_blocks, obs_count, near_tiles, taper_class
):
    members, levels, points = anomalies.shape
    owned = dual_rows.shape[0]
    tile = ("z", "y")
    raw = anomalies.reshape(members * levels, points)
    meta, own, weights, foot, duals = kernel(
        pack_body,
        [
            array((16,), jnp.int32),
            array((members + 16, levels * points), BF16),
            array(weighting.shape, F32),
            array(footprint.shape, BF16),
            array(dual_rows.shape, BF16),
        ],
        [near_tiles.T, obs_count, taper_class, raw, weighting, footprint, dual_rows],
        1e8,
        scratch=[
            pltpu.SMEM(near_tiles.T.shape, jnp.int32),
            pltpu.SMEM(obs_count.shape, jnp.int32),
            pltpu.SMEM(taper_class.shape, jnp.int32),
            pltpu.VMEM(raw.shape, BF16),
            pltpu.VMEM(raw.shape, F32),
            pltpu.SemaphoreType.DMA((7,)),
        ],
        given=[pltpu.HBM] * 7,
        spaces=[pltpu.SMEM] + [pltpu.VMEM] * 4,
    )
    other = move(own, "c", 1)

    rows = RELS * owned
    work = 2 * rows * points * members * levels
    (begun,) = kernel(
        own_body, [array((rows, members), F32)], [meta, foot, own, weights], work, scalars=1
    )
    (pay,) = kernel(
        other_body,
        [array((RELS, 3 * owned, members), BF16)],
        [meta, foot, other, begun, duals],
        work,
        scalars=1,
        scratch=[pltpu.VMEM((rows, members), F32)],
    )
    got = lax.all_to_all(pay, "x", 0, 0, tiled=True)
    (here,) = kernel(fold_body, [array((owned + rows, members), BF16)], [got], 1e8)
    low, high = move(here, tile, 1), move(here, tile, -1)
    y_mid = jnp.concatenate([a[:owned] for a in (low, here, high)], axis=0)
    y_low, y_high = move(y_mid, tile, 3), move(y_mid, tile, -3)
    w_mid = jnp.concatenate([a[owned:] for a in (low, here, high)], axis=0)
    w_low, w_high = move(w_mid, tile, 3), move(w_mid, tile, -3)
    (y0,) = kernel(
        pick_body,
        [array((NEAR * owned, members), BF16)],
        [meta, y_low, y_mid, y_high],
        1e8,
        scalars=1,
    )
    y3, y1, y2 = move(y0, "x", 1), move(y0, "x", -1), move(y0, "x", 2)

    taper_late, _ = lax.optimization_barrier((taper_blocks, y0))
    (scaled,) = kernel(
        taper_body,
        [array((RELS, NEAR * owned, points), F32)],
        [meta, taper_late],
        1e9,
        scalars=1,
        scratch=[pltpu.VMEM((taper_blocks.shape[0], taper_blocks.shape[2], points), F32)],
    )
    width = levels * points
    (flipped,) = kernel(
        flip_body,
        [array((members, NEAR * rows), BF16)],
        [meta, w_low, w_mid, w_high],
        1e9,
        scalars=1,
        scratch=[pltpu.VMEM((NEAR * owned, members), BF16)],
    )
    part = 2 * NEAR * owned * members * width
    tapered = None
    for place, got in ((0, y0), (1, y2)):
        (tapered,) = kernel(
            functools.partial(covary_body, place),
            [array((2 * NEAR * owned, 2 * width), BF16)],
            [got, own, other, scaled] + ([] if tapered is None else [tapered]),
            2 * part,
            aliases={} if tapered is None else {4: 0},
        )
    sums = kernel(gain_body, [array((members, width), F32)] * 2, [flipped, tapered], 4 * part)
    given, kept = (
        kernel(
            late_body,
            [array((members, width), kind)],
            [y3, y1, scaled, flipped, cells, before],
            4 * part,
        )[0]
        for kind, cells, before in ((BF16, other, sums[1]), (F32, own, sums[0]))
    )
    theirs = move(given, "c", 1)
    (out,) = kernel(
        finish_body,
        [array((members * levels, points), F32)],
        [kept, theirs],
        1e8,
        scratch=[pltpu.VMEM((members * levels, points), F32), pltpu.SemaphoreType.DMA((4,))],
        spaces=[None],
    )
    return out.reshape(members, levels, points)


def solution(mesh):
    fine = Mesh(mesh.devices.reshape(16, 4, 4, 2), ("z", "y", "x", "c"))
    tile, level = ("z", "y"), ("x", "c")
    return jax.shard_map(
        shards,
        mesh=fine,
        in_specs=(
            P(None, level, tile),
            P(tile, None),
            P(level, tile),
            P((*tile, *level), None),
            P(),
            P(),
            P(),
            P(tile, None),
        ),
        out_specs=P(None, level, tile),
        check_vma=False,
    )
```
